512 devices in a mesh: row: 64 (over x, y, core), col: 8 (over z).
Axes of the slice: x: 4, y: 8, z: 8, core: 2. Of those that a mesh axis runs over, the one named last changes fastest.
Arguments:
- matrix: float32 [16384, 4096], P('row', 'col'), may hold values from -7.8125 to 7.8125
Outputs:
- r_top: float32 [512, 4096], P(None, 'col')
- basis: float32 [16384, 512], P('row')
The draws below stay inside these ranges and needn't reach their ends.
All inputs are finite; a program needn't handle non-finite values.
Results may differ from the reference program's by a relative error of at most 0.0003.
Values sent between devices are 32-bit elements; how exact they have to be, the bound alone decides.
No kernel may reach another device: no remote copies, remote signals or barrier semaphores. Data moves between devices by JAX's collectives and lax.ppermute only.
A program may use at most 64 MiB of HBM per device.

```python
import math
import jax
import jax.numpy as jnp
from jax import lax

PANEL = 256
NCOLS = 4096
ROWS = 16384


def mixing(key, width, spread):
    keys = jax.random.split(key, 2)
    left, unused_left = jnp.linalg.qr(jax.random.normal(keys[0], (width, width), jnp.float32))
    right, unused_right = jnp.linalg.qr(jax.random.normal(keys[1], (width, width), jnp.float32))
    levels = jnp.exp(-math.log(spread) * jnp.arange(width, dtype=jnp.float32) / (width - 1))
    mixed = jnp.dot(left * levels[None, :], right.T, precision=lax.Precision.HIGHEST)
    return mixed / jnp.sqrt(jnp.sum(mixed * mixed, axis=0, keepdims=True))


def draw_matrix(key, part):
    base = jax.random.fold_in(key, 11)
    keys = jax.random.split(base, 11)
    noise = jnp.clip(jax.random.normal(keys[0], (ROWS, NCOLS), jnp.float32), -6.0, 6.0)
    shared = jnp.clip(jax.random.normal(keys[3], (ROWS, 1), jnp.float32), -3.0, 3.0)
    weights = jnp.clip(jax.random.normal(keys[4], (1, NCOLS), jnp.float32), -3.0, 3.0)
    spread = 4.0
    row_span = math.log(2.0)
    ramp_span = math.log(3.0)
    common = 0.0 * shared * weights
    first = jnp.dot(noise[:, :PANEL], mixing(keys[5], PANEL, spread), precision=lax.Precision.HIGHEST)
    second = jnp.dot(noise[:, PANEL:2 * PANEL], mixing(keys[6], PANEL, spread), precision=lax.Precision.HIGHEST)
    panels = jnp.clip(jnp.concatenate([first, second], axis=1), -8.0, 8.0)
    values = jnp.concatenate([panels, noise[:, 2 * PANEL:]], axis=1) + common
    ramp = jnp.exp(ramp_span * jnp.arange(ROWS, dtype=jnp.float32) / ROWS)
    row_scale = ramp * jnp.exp(jax.random.uniform(keys[1], (ROWS,), jnp.float32, 0.0, row_span))
    col_scale = jnp.exp(jax.random.uniform(keys[2], (NCOLS,), jnp.float32, 0.0, math.log(3.0)))
    values = values * row_scale[:, None] * col_scale[None, :] / math.sqrt(ROWS)
    bound = 1000.0 / math.sqrt(ROWS)
    row_high = jax.random.randint(keys[7], (), 0, ROWS)
    row_low = (row_high + jax.random.randint(keys[8], (), 1, ROWS)) % ROWS
    col_high = jax.random.randint(keys[9], (), 2 * PANEL, NCOLS)
    col_low = jax.random.randint(keys[10], (), 2 * PANEL, NCOLS)
    values = values.at[row_high, col_high].set(bound)
    values = values.at[row_low, col_low].set(-bound)
    return values.astype(jnp.float32)


def setup_inputs(seed: int = 0) -> dict:
    key_list = jax.random.split(jax.random.key(seed), 2)
    matrix = draw_matrix(jax.random.fold_in(key_list[1], 71), 0)
    return dict(matrix=matrix)


def signed_qr(panel):
    left, right = jnp.linalg.qr(panel)
    signs = jnp.sign(jnp.diagonal(right))
    return (left * signs[None, :], right * signs[:, None])

def reference(matrix):
    highest = lax.Precision.HIGHEST
    panel_cols = PANEL
    q_first, r_first = signed_qr(matrix[:, :panel_cols])
    z_first = jnp.dot(q_first.T, matrix[:, panel_cols:], precision=highest)
    second = matrix[:, panel_cols:2 * panel_cols] - jnp.dot(q_first, z_first[:, :panel_cols], precision=highest)
    q_second, r_second = signed_qr(second)
    cross = jnp.dot(q_second.T, q_first, precision=highest)
    z_second = jnp.dot(q_second.T, matrix[:, 2 * panel_cols:], precision=highest) - jnp.dot(cross, z_first[:, panel_cols:], precision=highest)
    zeros = jnp.zeros((panel_cols, panel_cols), jnp.float32)
    top = jnp.concatenate([jnp.concatenate([r_first, z_first], axis=1), jnp.concatenate([zeros, r_second, z_second], axis=1)], axis=0)
    basis = jnp.concatenate([q_first, q_second], axis=1) * math.sqrt(ROWS)
    return (top, basis)
```

```python
import math

import jax
import jax.numpy as jnp
from jax import lax
from jax.experimental import pallas as pl
from jax.experimental.pallas import tpu as pltpu
from jax.sharding import Mesh
from jax.sharding import PartitionSpec as P

PANEL = 256
WIDE = 2 * PANEL
TILE = 128
STEP = 32
ROW = ("x", "y", "core")
PLANE = ("x", "y")
HIGHEST = lax.Precision.HIGHEST


def inner(left, right):
    return lax.dot_general(
        left,
        right,
        (((0,), (0,)), ((), ())),
        precision=HIGHEST,
        preferred_element_type=jnp.float32,
    )


def product(left, right):
    return jnp.dot(left, right, precision=HIGHEST, preferred_element_type=jnp.float32)


PLACES = {0: (0, 0), 3: (0, 4), 1: (1, 0), 2: (1, 3)}


def packed_gram(panels):
    rows = {}
    for i in range(4):
        rows[i] = inner(panels[:, i * TILE : (i + 1) * TILE], panels[:, i * TILE :])
    return jnp.concatenate(
        [jnp.concatenate([rows[0], rows[3]], 1), jnp.concatenate([rows[1], rows[2]], 1)], 0
    )


def factor_kernel(packed_ref, out_ref):
    row8 = lax.broadcasted_iota(jnp.int32, (8, TILE), 0)
    lane = lax.broadcasted_iota(jnp.int32, (8, TILE), 1)
    tiles, groups = WIDE // TILE, STEP // 8
    for i, (r, c) in PLACES.items():
        out_ref[i * TILE : (i + 1) * TILE, i * TILE :] = packed_ref[
            r * TILE : (r + 1) * TILE, c * TILE : (c + 4 - i) * TILE
        ]

    def outer(t, _):
        base = pl.multiple_of(t * TILE, TILE)
        for u in range(TILE // STEP):
            first = pl.multiple_of(base + u * STEP, STEP)
            block = out_ref[pl.ds(first, STEP), pl.ds(base, TILE)]
            cols = []
            for q in range(STEP):
                spread = jnp.broadcast_to(block[:, u * STEP + q : u * STEP + q + 1], (STEP, TILE))
                cols.append([spread[8 * v : 8 * v + 8] for v in range(groups)])
            rows = []
            for v in range(groups):
                rows.append([])
                for w in range(tiles):
                    values = out_ref[pl.ds(first + 8 * v, 8), TILE * w : TILE * (w + 1)]
                    here = (lane >= u * STEP) & (lane < (u + 1) * STEP) & (t == w)
                    unit = jnp.where(lane - u * STEP == row8 + 8 * v, 1.0, 0.0)
                    rows[v].append(jnp.where(here, unit, values))
            pivots = [None] * groups
            for k in range(STEP):
                vk, sk = k // 8, k % 8
                pivot = jnp.broadcast_to(cols[k][vk][sk : sk + 1], (8, TILE))
                inverse = 1.0 / pivot
                pivots[vk] = pivot if sk == 0 else jnp.where(row8 == sk, pivot, pivots[vk])
                scaled = {}
                for v in range(vk, groups):
                    s = cols[k][v] * inverse
                    scaled[v] = jnp.where(row8 > sk, s, 0.0) if v == vk else s
                for j in range(k + 1, STEP):
                    other = jnp.broadcast_to(cols[k][j // 8][j % 8 : j % 8 + 1], (8, TILE))
                    for v in range(j // 8, groups):
                        cols[j][v] = cols[j][v] - scaled[v] * other
                for w in range(tiles):
                    other = jnp.broadcast_to(rows[vk][w][sk : sk + 1], (8, TILE))
                    for v in range(vk, groups):
                        rows[v][w] = rows[v][w] - scaled[v] * other
            for v in range(groups):
                scale = lax.rsqrt(pivots[v])
                for w in range(tiles):
                    out_ref[pl.ds(first + 8 * v, 8), TILE * w : TILE * (w + 1)] = rows[v][w] * scale
            if u < TILE // STEP - 1:
                rest = TILE - (u + 1) * STEP
                done = out_ref[pl.ds(first, STEP), :]
                left = out_ref[pl.ds(first, STEP), pl.ds(base, TILE)][:, (u + 1) * STEP :]
                old = out_ref[pl.ds(first + STEP, rest), :]
                col = lax.broadcasted_iota(jnp.int32, (rest, WIDE), 1)
                old = jnp.where((col >= first) & (col < first + STEP), 0.0, old)
                out_ref[pl.ds(first + STEP, rest), :] = old - inner(left, done)

        done = out_ref[pl.ds(base, TILE), :]
        row = lax.broadcasted_iota(jnp.int32, (TILE, WIDE), 0) + base
        col = lax.broadcasted_iota(jnp.int32, (TILE, WIDE), 1)
        done = jnp.where((col <= row) | (col >= base + TILE), done, 0.0)

        def below(i, _):
            start = pl.multiple_of(i * TILE, TILE)
            old = out_ref[pl.ds(start, TILE), :]
            old = jnp.where((col >= base) & (col < base + TILE), 0.0, old)
            out_ref[pl.ds(start, TILE), :] = old - inner(
                out_ref[pl.ds(base, TILE), pl.ds(start, TILE)], done
            )
            return 0

        lax.fori_loop(t + 1, tiles, below, 0)
        return 0

    lax.fori_loop(0, tiles, outer, 0)
    row = lax.broadcasted_iota(jnp.int32, (WIDE, WIDE), 0)
    col = lax.broadcasted_iota(jnp.int32, (WIDE, WIDE), 1)
    out_ref[...] = jnp.where(col <= row, out_ref[...], 0.0)


def inverse_factor(packed):
    vmem = pl.BlockSpec(memory_space=pltpu.VMEM)
    return pl.pallas_call(
        factor_kernel,
        out_shape=jax.ShapeDtypeStruct((WIDE, WIDE), jnp.float32),
        in_specs=[vmem],
        out_specs=vmem,
        compiler_params=pltpu.CompilerParams(vmem_limit_bytes=16 * 2**20),
        cost_estimate=pl.CostEstimate(
            flops=2_000_000_000, bytes_accessed=2**21, transcendentals=0
        ),
    )(packed)


def exchange(blocks, axis):
    return lax.all_to_all(blocks, axis, 0, 0, tiled=True)


def copies(array, axis):
    return exchange(jnp.broadcast_to(array[None], (lax.axis_size(axis), *array.shape)), axis)


def scattered_sum(array):
    width = array.shape[1]
    half = exchange(array.reshape(2, -1, width), "core").sum(axis=0)
    chips = lax.axis_size(PLANE)
    return exchange(half.reshape(chips, -1, width), PLANE).sum(axis=0)


def gathered(part):
    half = copies(part, PLANE).reshape(-1, part.shape[1])
    return copies(half, "core").reshape(-1, part.shape[1])


def body(matrix):
    rows_all = matrix.shape[0] * lax.axis_size(ROW)
    blocks = lax.axis_size("col")
    gram_part = scattered_sum(packed_gram(matrix))
    own = exchange(matrix.reshape(blocks, -1, WIDE), "col")[0]
    panels = copies(own, "col").reshape(-1, WIDE)
    gram_part = copies(gram_part, "col")[0]
    gram = gathered(gram_part)
    inner_products = gathered(scattered_sum(inner(panels, matrix)))
    inverse = inverse_factor(gram)
    top = product(inverse, inner_products)
    row = lax.broadcasted_iota(jnp.int32, (WIDE, WIDE), 0)
    column = lax.broadcasted_iota(jnp.int32, (WIDE, WIDE), 1)
    top = jnp.where((row > column) & (lax.axis_index("col") == 0), 0.0, top)
    basis = product(panels, inverse.T) * math.sqrt(rows_all)
    return (top, basis)


def solution(mesh):
    finer = Mesh(
        mesh.devices.reshape(4, 8, 2, mesh.shape["col"]), ("x", "y", "core", "col")
    )
    return jax.shard_map(
        body,
        mesh=finer,
        in_specs=(P(ROW, "col"),),
        out_specs=(P(None, "col"), P(ROW, None)),
        check_vma=False,
    )
```

```python
import math

import jax
import jax.numpy as jnp
from jax import lax
from jax.experimental import pallas as pl
from jax.experimental.pallas import tpu as pltpu
from jax.sharding import Mesh
from jax.sharding import PartitionSpec as P

PANEL = 256
WIDE = 2 * PANEL
TILE = 128
STEP = 32
ROW = ("x", "y", "core")
PLANE = ("x", "y")
HIGHEST = lax.Precision.HIGHEST


def inner(left, right):
    return lax.dot_general(
        left,
        right,
        (((0,), (0,)), ((), ())),
        precision=HIGHEST,
        preferred_element_type=jnp.float32,
    )


def product(left, right):
    return jnp.dot(left, right, precision=HIGHEST, preferred_element_type=jnp.float32)


SLOTS = 3
PLACES = {
    (i, j): (n // SLOTS, n % SLOTS)
    for n, (i, j) in enumerate((i, j) for i in range(4) for j in range(i, 4))
}


def blocks_of(place):
    return tuple(slice(p * TILE, (p + 1) * TILE) for p in place)


def gram_kernel(panels_ref, out_ref):
    for i in range(4):
        left = panels_ref[:, i * TILE : (i + 1) * TILE]
        line = inner(left, panels_ref[:, i * TILE :])
        for j in range(i, 4):
            out_ref[blocks_of(PLACES[i, j])] = line[:, (j - i) * TILE : (j - i + 1) * TILE]
    for n in range(len(PLACES), 4 * SLOTS):
        out_ref[blocks_of((n // SLOTS, n % SLOTS))] = jnp.zeros((TILE, TILE), jnp.float32)


def packed_gram(panels):
    vmem = pl.BlockSpec(memory_space=pltpu.VMEM)
    return pl.pallas_call(
        gram_kernel,
        out_shape=jax.ShapeDtypeStruct((WIDE, SLOTS * TILE), jnp.float32),
        in_specs=[vmem],
        out_specs=vmem,
        compiler_params=pltpu.CompilerParams(vmem_limit_bytes=16 * 2**20),
        cost_estimate=pl.CostEstimate(flops=600_000_000, bytes_accessed=2**20, transcendentals=0),
    )(panels)


def factor_kernel(core_ref, own_ref, other_ref, out_ref):
    row8 = lax.broadcasted_iota(jnp.int32, (8, TILE), 0)
    lane = lax.broadcasted_iota(jnp.int32, (8, TILE), 1)
    tiles, groups = WIDE // TILE, STEP // 8
    for half in range(2):

        def take(ref):
            for (i, j), (r, c) in PLACES.items():
                if r // 2 == half:
                    out_ref[blocks_of((i, j))] = ref[blocks_of((r % 2, c))]

        @pl.when(core_ref[0] == half)
        def _():
            take(own_ref)

        @pl.when(core_ref[0] != half)
        def _():
            take(other_ref)

    def outer(t, _):
        base = pl.multiple_of(t * TILE, TILE)
        for u in range(TILE // STEP):
            first = pl.multiple_of(base + u * STEP, STEP)
            block = out_ref[pl.ds(first, STEP), pl.ds(base, TILE)]
            cols = []
            for q in range(STEP):
                spread = jnp.broadcast_to(block[:, u * STEP + q : u * STEP + q + 1], (STEP, TILE))
                cols.append([spread[8 * v : 8 * v + 8] for v in range(groups)])
            rows = []
            for v in range(groups):
                rows.append([])
                for w in range(tiles):
                    values = out_ref[pl.ds(first + 8 * v, 8), TILE * w : TILE * (w + 1)]
                    here = (lane >= u * STEP) & (lane < (u + 1) * STEP) & (t == w)
                    unit = jnp.where(lane - u * STEP == row8 + 8 * v, 1.0, 0.0)
                    rows[v].append(jnp.where(here, unit, values))
            pivots = [None] * groups
            for k in range(STEP):
                vk, sk = k // 8, k % 8
                pivot = jnp.broadcast_to(cols[k][vk][sk : sk + 1], (8, TILE))
                inverse = 1.0 / pivot
                pivots[vk] = pivot if sk == 0 else jnp.where(row8 == sk, pivot, pivots[vk])
                scaled = {}
                for v in range(vk, groups):
                    s = cols[k][v] * inverse
                    scaled[v] = jnp.where(row8 > sk, s, 0.0) if v == vk else s
                for j in range(k + 1, STEP):
                    other = jnp.broadcast_to(cols[k][j // 8][j % 8 : j % 8 + 1], (8, TILE))
                    for v in range(j // 8, groups):
                        cols[j][v] = cols[j][v] - scaled[v] * other
                for w in range(tiles):
                    other = jnp.broadcast_to(rows[vk][w][sk : sk + 1], (8, TILE))
                    for v in range(vk, groups):
                        rows[v][w] = rows[v][w] - scaled[v] * other
            for v in range(groups):
                scale = lax.rsqrt(pivots[v])
                for w in range(tiles):
                    out_ref[pl.ds(first + 8 * v, 8), TILE * w : TILE * (w + 1)] = rows[v][w] * scale
            if u < TILE // STEP - 1:
                rest = TILE - (u + 1) * STEP
                done = out_ref[pl.ds(first, STEP), :]
                left = out_ref[pl.ds(first, STEP), pl.ds(base, TILE)][:, (u + 1) * STEP :]
                old = out_ref[pl.ds(first + STEP, rest), :]
                col = lax.broadcasted_iota(jnp.int32, (rest, WIDE), 1)
                old = jnp.where((col >= first) & (col < first + STEP), 0.0, old)
                out_ref[pl.ds(first + STEP, rest), :] = old - inner(left, done)

        done = out_ref[pl.ds(base, TILE), :]
        row = lax.broadcasted_iota(jnp.int32, (TILE, WIDE), 0) + base
        col = lax.broadcasted_iota(jnp.int32, (TILE, WIDE), 1)
        done = jnp.where((col <= row) | (col >= base + TILE), done, 0.0)

        def below(i, _):
            start = pl.multiple_of(i * TILE, TILE)
            old = out_ref[pl.ds(start, TILE), :]
            old = jnp.where((col >= base) & (col < base + TILE), 0.0, old)
            out_ref[pl.ds(start, TILE), :] = old - inner(
                out_ref[pl.ds(base, TILE), pl.ds(start, TILE)], done
            )
            return 0

        lax.fori_loop(t + 1, tiles, below, 0)
        return 0

    lax.fori_loop(0, tiles, outer, 0)
    row = lax.broadcasted_iota(jnp.int32, (WIDE, WIDE), 0)
    col = lax.broadcasted_iota(jnp.int32, (WIDE, WIDE), 1)
    out_ref[...] = jnp.where(col <= row, out_ref[...], 0.0)


def inverse_factor(core, own, other):
    vmem = pl.BlockSpec(memory_space=pltpu.VMEM)
    return pl.pallas_call(
        factor_kernel,
        out_shape=jax.ShapeDtypeStruct((WIDE, WIDE), jnp.float32),
        in_specs=[pl.BlockSpec(memory_space=pltpu.SMEM), vmem, vmem],
        out_specs=vmem,
        compiler_params=pltpu.CompilerParams(vmem_limit_bytes=16 * 2**20),
        cost_estimate=pl.CostEstimate(
            flops=2_000_000_000, bytes_accessed=2**21, transcendentals=0
        ),
    )(core.reshape(1), own, other)


def exchange(blocks, axis):
    return lax.all_to_all(blocks, axis, 0, 0, tiled=True)


def spread(array, count):
    return jnp.broadcast_to(array[None], (count, *array.shape))


def from_root(pieces, own):
    arrived = jnp.where(lax.axis_index("col") == 0, own, 0.0)
    for k in range(1, lax.axis_size("col")):
        arrived = arrived + lax.ppermute(pieces(k), "col", [(0, k)])
    return arrived


def core_sum(array):
    return exchange(array.reshape(2, -1, array.shape[1]), "core").sum(axis=0)


def body(matrix):
    rows_all = matrix.shape[0] * lax.axis_size(ROW)
    devices = lax.axis_size("col")
    chips = lax.axis_size(PLANE)
    lines = matrix.shape[0] // devices
    narrow = SLOTS * TILE
    core = lax.axis_index("core")

    piece = from_root(lambda k: matrix[k * lines : (k + 1) * lines], matrix[:lines])
    half = core_sum(packed_gram(matrix))
    gram_part = exchange(half.reshape(chips, -1, narrow), PLANE).sum(axis=0)
    gram_part = from_root(lambda k: gram_part, gram_part)
    panels = exchange(spread(piece, devices), "col").reshape(-1, WIDE)

    half = core_sum(inner(panels, matrix)).reshape(chips, -1, WIDE)
    both = jnp.concatenate([half, spread(gram_part, chips)], axis=2)
    both = exchange(both, PLANE)
    part = both[:, :, :WIDE].sum(axis=0)
    own = both[:, :, WIDE:].reshape(-1, narrow)
    other = lax.ppermute(own, "core", [(0, 1), (1, 0)])

    half = exchange(spread(part, chips), PLANE).reshape(-1, WIDE)
    inner_products = exchange(spread(half, 2), "core").reshape(-1, WIDE)
    inverse = inverse_factor(core, own, other)
    top = product(inverse, inner_products)
    row = lax.broadcasted_iota(jnp.int32, (WIDE, WIDE), 0)
    column = lax.broadcasted_iota(jnp.int32, (WIDE, WIDE), 1)
    top = jnp.where((row > column) & (lax.axis_index("col") == 0), 0.0, top)
    basis = product(panels, inverse.T) * math.sqrt(rows_all)
    return (top, basis)


def solution(mesh):
    finer = Mesh(
        mesh.devices.reshape(4, 8, 2, mesh.shape["col"]), ("x", "y", "core", "col")
    )
    return jax.shard_map(
        body,
        mesh=finer,
        in_specs=(P(ROW, "col"),),
        out_specs=(P(None, "col"), P(ROW, None)),
        check_vma=False,
    )
```

```python
import math

import jax
import jax.numpy as jnp
from jax import lax
from jax.experimental import pallas as pl
from jax.experimental.pallas import tpu as pltpu
from jax.sharding import Mesh
from jax.sharding import PartitionSpec as P

PANEL = 256
WIDE = 2 * PANEL
TILE = 128
STEP = 32
ROW = ("x", "y", "core")
PLANE = ("x", "y")
HIGHEST = lax.Precision.HIGHEST


def inner(left, right):
    return lax.dot_general(
        left,
        right,
        (((0,), (0,)), ((), ())),
        precision=HIGHEST,
        preferred_element_type=jnp.float32,
    )


def product(left, right):
    return jnp.dot(left, right, precision=HIGHEST, preferred_element_type=jnp.float32)


SLOTS = 3
PLACES = {
    (i, j): (n // SLOTS, n % SLOTS)
    for n, (i, j) in enumerate((i, j) for i in range(4) for j in range(i, 4))
}


def blocks_of(place):
    return tuple(slice(p * TILE, (p + 1) * TILE) for p in place)


def gram_kernel(panels_ref, out_ref):
    for i in range(4):
        left = panels_ref[:, i * TILE : (i + 1) * TILE]
        line = inner(left, panels_ref[:, i * TILE :])
        for j in range(i, 4):
            out_ref[blocks_of(PLACES[i, j])] = line[:, (j - i) * TILE : (j - i + 1) * TILE]
    for n in range(len(PLACES), 4 * SLOTS):
        out_ref[blocks_of((n // SLOTS, n % SLOTS))] = jnp.zeros((TILE, TILE), jnp.float32)


def packed_gram(panels):
    vmem = pl.BlockSpec(memory_space=pltpu.VMEM)
    return pl.pallas_call(
        gram_kernel,
        out_shape=jax.ShapeDtypeStruct((WIDE, SLOTS * TILE), jnp.float32),
        in_specs=[vmem],
        out_specs=vmem,
        compiler_params=pltpu.CompilerParams(vmem_limit_bytes=16 * 2**20),
        cost_estimate=pl.CostEstimate(flops=600_000_000, bytes_accessed=2**20, transcendentals=0),
    )(panels)


def factor_kernel(core_ref, own_ref, other_ref, out_ref):
    row8 = lax.broadcasted_iota(jnp.int32, (8, TILE), 0)
    lane = lax.broadcasted_iota(jnp.int32, (8, TILE), 1)
    tiles, groups = WIDE // TILE, STEP // 8
    for half in range(2):

        def take(ref):
            for (i, j), (r, c) in PLACES.items():
                if r // 2 == half:
                    out_ref[blocks_of((i, j))] = ref[blocks_of((r % 2, c))]

        @pl.when(core_ref[0] == half)
        def _():
            take(own_ref)

        @pl.when(core_ref[0] != half)
        def _():
            take(other_ref)

    def outer(t, _):
        base = pl.multiple_of(t * TILE, TILE)
        for u in range(TILE // STEP):
            first = pl.multiple_of(base + u * STEP, STEP)
            block = out_ref[pl.ds(first, STEP), pl.ds(base, TILE)]
            cols = []
            for q in range(STEP):
                spread = jnp.broadcast_to(block[:, u * STEP + q : u * STEP + q + 1], (STEP, TILE))
                cols.append([spread[8 * v : 8 * v + 8] for v in range(groups)])
            rows = []
            for v in range(groups):
                rows.append([])
                for w in range(tiles):
                    values = out_ref[pl.ds(first + 8 * v, 8), TILE * w : TILE * (w + 1)]
                    here = (lane >= u * STEP) & (lane < (u + 1) * STEP) & (t == w)
                    unit = jnp.where(lane - u * STEP == row8 + 8 * v, 1.0, 0.0)
                    rows[v].append(jnp.where(here, unit, values))
            pivots = [None] * groups
            for k in range(STEP):
                vk, sk = k // 8, k % 8
                pivot = jnp.broadcast_to(cols[k][vk][sk : sk + 1], (8, TILE))
                inverse = 1.0 / pivot
                pivots[vk] = pivot if sk == 0 else jnp.where(row8 == sk, pivot, pivots[vk])
                scaled = {}
                for v in range(vk, groups):
                    s = cols[k][v] * inverse
                    scaled[v] = jnp.where(row8 > sk, s, 0.0) if v == vk else s
                for j in range(k + 1, STEP):
                    other = jnp.broadcast_to(cols[k][j // 8][j % 8 : j % 8 + 1], (8, TILE))
                    for v in range(j // 8, groups):
                        cols[j][v] = cols[j][v] - scaled[v] * other
                for w in range(tiles):
                    other = jnp.broadcast_to(rows[vk][w][sk : sk + 1], (8, TILE))
                    for v in range(vk, groups):
                        rows[v][w] = rows[v][w] - scaled[v] * other
            for v in range(groups):
                scale = lax.rsqrt(pivots[v])
                for w in range(tiles):
                    out_ref[pl.ds(first + 8 * v, 8), TILE * w : TILE * (w + 1)] = rows[v][w] * scale
            if u < TILE // STEP - 1:
                rest = TILE - (u + 1) * STEP
                done = out_ref[pl.ds(first, STEP), :]
                left = out_ref[pl.ds(first, STEP), pl.ds(base, TILE)][:, (u + 1) * STEP :]
                old = out_ref[pl.ds(first + STEP, rest), :]
                col = lax.broadcasted_iota(jnp.int32, (rest, WIDE), 1)
                old = jnp.where((col >= first) & (col < first + STEP), 0.0, old)
                out_ref[pl.ds(first + STEP, rest), :] = old - inner(left, done)

        done = out_ref[pl.ds(base, TILE), :]
        row = lax.broadcasted_iota(jnp.int32, (TILE, WIDE), 0) + base
        col = lax.broadcasted_iota(jnp.int32, (TILE, WIDE), 1)
        done = jnp.where((col <= row) | (col >= base + TILE), done, 0.0)

        def below(i, _):
            start = pl.multiple_of(i * TILE, TILE)
            old = out_ref[pl.ds(start, TILE), :]
            old = jnp.where((col >= base) & (col < base + TILE), 0.0, old)
            out_ref[pl.ds(start, TILE), :] = old - inner(
                out_ref[pl.ds(base, TILE), pl.ds(start, TILE)], done
            )
            return 0

        lax.fori_loop(t + 1, tiles, below, 0)
        return 0

    lax.fori_loop(0, tiles, outer, 0)
    row = lax.broadcasted_iota(jnp.int32, (WIDE, WIDE), 0)
    col = lax.broadcasted_iota(jnp.int32, (WIDE, WIDE), 1)
    out_ref[...] = jnp.where(col <= row, out_ref[...], 0.0)


def inverse_factor(core, own, other):
    vmem = pl.BlockSpec(memory_space=pltpu.VMEM)
    return pl.pallas_call(
        factor_kernel,
        out_shape=jax.ShapeDtypeStruct((WIDE, WIDE), jnp.float32),
        in_specs=[pl.BlockSpec(memory_space=pltpu.SMEM), vmem, vmem],
        out_specs=vmem,
        compiler_params=pltpu.CompilerParams(vmem_limit_bytes=16 * 2**20),
        cost_estimate=pl.CostEstimate(
            flops=2_000_000_000, bytes_accessed=2**21, transcendentals=0
        ),
    )(core.reshape(1), own, other)


def exchange(blocks, axis):
    return lax.all_to_all(blocks, axis, 0, 0, tiled=True)


def spread(array, count):
    return jnp.broadcast_to(array[None], (count, *array.shape))


def scattered(pieces, own):
    arrived = jnp.where(lax.axis_index("col") == 0, own, 0.0)
    for k in range(1, lax.axis_size("col")):
        arrived = arrived + lax.ppermute(pieces(k), "col", [(0, k)])
    return arrived


def swapped(array):
    return lax.ppermute(array, "core", [(0, 1), (1, 0)])


def body(matrix):
    rows_all = matrix.shape[0] * lax.axis_size(ROW)
    devices = lax.axis_size("col")
    chips = lax.axis_size(PLANE)
    lines = matrix.shape[0] // devices
    narrow = SLOTS * TILE
    core = lax.axis_index("core")

    piece = scattered(lambda k: matrix[k * lines : (k + 1) * lines], matrix[:lines])
    half = exchange(packed_gram(matrix).reshape(2, -1, narrow), "core").sum(axis=0)
    gram_part = exchange(half.reshape(chips, -1, narrow), PLANE).sum(axis=0)
    extra = jnp.pad(gram_part, ((0, 0), (0, WIDE - narrow)))
    both = exchange(spread(jnp.concatenate([piece, extra], axis=0), devices), "col")
    panels = both[:, :lines].reshape(-1, WIDE)
    gram_part = both[0, lines:, :narrow]

    own = exchange(spread(gram_part, chips), PLANE).reshape(-1, narrow)
    products = inner(panels, matrix).reshape(2, -1, WIDE)
    mine = jnp.where(core == 0, products[0], products[1])
    half = mine + swapped(jnp.where(core == 0, products[1], products[0]))
    inverse = inverse_factor(core, own, swapped(own))
    half, _ = lax.optimization_barrier((half, own))
    part = exchange(half.reshape(chips, -1, WIDE), PLANE).sum(axis=0)
    half = exchange(spread(part, chips), PLANE).reshape(-1, WIDE)
    inner_products = exchange(spread(half, 2), "core").reshape(-1, WIDE)
    top = product(inverse, inner_products)
    row = lax.broadcasted_iota(jnp.int32, (WIDE, WIDE), 0)
    column = lax.broadcasted_iota(jnp.int32, (WIDE, WIDE), 1)
    top = jnp.where((row > column) & (lax.axis_index("col") == 0), 0.0, top)
    basis = product(panels, inverse.T) * math.sqrt(rows_all)
    return (top, basis)


def solution(mesh):
    finer = Mesh(
        mesh.devices.reshape(4, 8, 2, mesh.shape["col"]), ("x", "y", "core", "col")
    )
    return jax.shard_map(
        body,
        mesh=finer,
        in_specs=(P(ROW, "col"),),
        out_specs=(P(None, "col"), P(ROW, None)),
        check_vma=False,
    )
```

```python
import math

import jax
import jax.numpy as jnp
from jax import lax
from jax.experimental import pallas as pl
from jax.experimental.pallas import tpu as pltpu
from jax.sharding import Mesh
from jax.sharding import PartitionSpec as P

PANEL = 256
WIDE = 2 * PANEL
TILE = 128
STEP = 32
ROW = ("x", "y", "core")
PLANE = ("x", "y")
HIGHEST = lax.Precision.HIGHEST


def inner(left, right):
    return lax.dot_general(
        left,
        right,
        (((0,), (0,)), ((), ())),
        precision=HIGHEST,
        preferred_element_type=jnp.float32,
    )


def product(left, right):
    return jnp.dot(left, right, precision=HIGHEST, preferred_element_type=jnp.float32)


SLOTS = 3
PLACES = {
    (i, j): (n // SLOTS, n % SLOTS)
    for n, (i, j) in enumerate((i, j) for i in range(4) for j in range(i, 4))
}


def blocks_of(place):
    return tuple(slice(p * TILE, (p + 1) * TILE) for p in place)


def gram_kernel(panels_ref, out_ref):
    for i in range(4):
        left = panels_ref[:, i * TILE : (i + 1) * TILE]
        line = inner(left, panels_ref[:, i * TILE :])
        for j in range(i, 4):
            out_ref[blocks_of(PLACES[i, j])] = line[:, (j - i) * TILE : (j - i + 1) * TILE]
    for n in range(len(PLACES), 4 * SLOTS):
        out_ref[blocks_of((n // SLOTS, n % SLOTS))] = jnp.zeros((TILE, TILE), jnp.float32)


def packed_gram(panels):
    vmem = pl.BlockSpec(memory_space=pltpu.VMEM)
    return pl.pallas_call(
        gram_kernel,
        out_shape=jax.ShapeDtypeStruct((WIDE, SLOTS * TILE), jnp.float32),
        in_specs=[vmem],
        out_specs=vmem,
        compiler_params=pltpu.CompilerParams(vmem_limit_bytes=16 * 2**20),
        cost_estimate=pl.CostEstimate(flops=600_000_000, bytes_accessed=2**20, transcendentals=0),
    )(panels)


def factor_kernel(core_ref, own_ref, other_ref, out_ref):
    row8 = lax.broadcasted_iota(jnp.int32, (8, TILE), 0)
    lane = lax.broadcasted_iota(jnp.int32, (8, TILE), 1)
    tiles, groups = WIDE // TILE, STEP // 8
    for half in range(2):

        def take(ref):
            for (i, j), (r, c) in PLACES.items():
                if r // 2 == half:
                    out_ref[blocks_of((i, j))] = ref[blocks_of((r % 2, c))]

        @pl.when(core_ref[0] == half)
        def _():
            take(own_ref)

        @pl.when(core_ref[0] != half)
        def _():
            take(other_ref)

    def outer(t, _):
        base = pl.multiple_of(t * TILE, TILE)
        for u in range(TILE // STEP):
            first = pl.multiple_of(base + u * STEP, STEP)
            block = out_ref[pl.ds(first, STEP), pl.ds(base, TILE)]
            cols = []
            for q in range(STEP):
                spread = jnp.broadcast_to(block[:, u * STEP + q : u * STEP + q + 1], (STEP, TILE))
                cols.append([spread[8 * v : 8 * v + 8] for v in range(groups)])
            rows = []
            for v in range(groups):
                rows.append([])
                for w in range(tiles):
                    values = out_ref[pl.ds(first + 8 * v, 8), TILE * w : TILE * (w + 1)]
                    here = (lane >= u * STEP) & (lane < (u + 1) * STEP) & (t == w)
                    unit = jnp.where(lane - u * STEP == row8 + 8 * v, 1.0, 0.0)
                    rows[v].append(jnp.where(here, unit, values))
            pivots = [None] * groups
            for k in range(STEP):
                vk, sk = k // 8, k % 8
                pivot = jnp.broadcast_to(cols[k][vk][sk : sk + 1], (8, TILE))
                inverse = 1.0 / pivot
                pivots[vk] = pivot if sk == 0 else jnp.where(row8 == sk, pivot, pivots[vk])
                scaled = {}
                for v in range(vk, groups):
                    s = cols[k][v] * inverse
                    scaled[v] = jnp.where(row8 > sk, s, 0.0) if v == vk else s
                for j in range(k + 1, STEP):
                    other = jnp.broadcast_to(cols[k][j // 8][j % 8 : j % 8 + 1], (8, TILE))
                    for v in range(j // 8, groups):
                        cols[j][v] = cols[j][v] - scaled[v] * other
                for w in range(tiles):
                    other = jnp.broadcast_to(rows[vk][w][sk : sk + 1], (8, TILE))
                    for v in range(vk, groups):
                        rows[v][w] = rows[v][w] - scaled[v] * other
            for v in range(groups):
                scale = lax.rsqrt(pivots[v])
                for w in range(tiles):
                    out_ref[pl.ds(first + 8 * v, 8), TILE * w : TILE * (w + 1)] = rows[v][w] * scale
            if u < TILE // STEP - 1:
                rest = TILE - (u + 1) * STEP
                done = out_ref[pl.ds(first, STEP), :]
                left = out_ref[pl.ds(first, STEP), pl.ds(base, TILE)][:, (u + 1) * STEP :]
                old = out_ref[pl.ds(first + STEP, rest), :]
                col = lax.broadcasted_iota(jnp.int32, (rest, WIDE), 1)
                old = jnp.where((col >= first) & (col < first + STEP), 0.0, old)
                out_ref[pl.ds(first + STEP, rest), :] = old - inner(left, done)

        done = out_ref[pl.ds(base, TILE), :]
        row = lax.broadcasted_iota(jnp.int32, (TILE, WIDE), 0) + base
        col = lax.broadcasted_iota(jnp.int32, (TILE, WIDE), 1)
        done = jnp.where((col <= row) | (col >= base + TILE), done, 0.0)

        def below(i, _):
            start = pl.multiple_of(i * TILE, TILE)
            old = out_ref[pl.ds(start, TILE), :]
            old = jnp.where((col >= base) & (col < base + TILE), 0.0, old)
            out_ref[pl.ds(start, TILE), :] = old - inner(
                out_ref[pl.ds(base, TILE), pl.ds(start, TILE)], done
            )
            return 0

        lax.fori_loop(t + 1, tiles, below, 0)
        return 0

    lax.fori_loop(0, tiles, outer, 0)
    row = lax.broadcasted_iota(jnp.int32, (WIDE, WIDE), 0)
    col = lax.broadcasted_iota(jnp.int32, (WIDE, WIDE), 1)
    out_ref[...] = jnp.where(col <= row, out_ref[...], 0.0)


def inverse_factor(core, own, other):
    vmem = pl.BlockSpec(memory_space=pltpu.VMEM)
    return pl.pallas_call(
        factor_kernel,
        out_shape=jax.ShapeDtypeStruct((WIDE, WIDE), jnp.float32),
        in_specs=[pl.BlockSpec(memory_space=pltpu.SMEM), vmem, vmem],
        out_specs=vmem,
        compiler_params=pltpu.CompilerParams(vmem_limit_bytes=16 * 2**20),
        cost_estimate=pl.CostEstimate(
            flops=2_000_000_000, bytes_accessed=2**21, transcendentals=0
        ),
    )(core.reshape(1), own, other)


def exchange(blocks, axis):
    return lax.all_to_all(blocks, axis, 0, 0, tiled=True)


def spread(array, count):
    return jnp.broadcast_to(array[None], (count, *array.shape))


def from_root(pieces, own):
    arrived = jnp.where(lax.axis_index("col") == 0, own, 0.0)
    for k in range(1, lax.axis_size("col")):
        arrived = arrived + lax.ppermute(pieces(k), "col", [(0, k)])
    return arrived


def swapped(array):
    return lax.ppermute(array, "core", [(0, 1), (1, 0)])


def ring_sum(array):
    count, me = lax.axis_size("x"), lax.axis_index("x")
    parts = array.reshape(count, -1, array.shape[1])
    total = lax.dynamic_index_in_dim(parts, me, 0, keepdims=False)
    for step in range(1, count):
        there = lax.rem(me + step, count)
        sent = lax.dynamic_index_in_dim(parts, there, 0, keepdims=False)
        total = total + lax.ppermute(sent, "x", [(i, (i + step) % count) for i in range(count)])
    return total


def body(matrix):
    rows_all = matrix.shape[0] * lax.axis_size(ROW)
    devices = lax.axis_size("col")
    chips = lax.axis_size(PLANE)
    lines = matrix.shape[0] // devices
    narrow = SLOTS * TILE
    core = lax.axis_index("core")

    piece = from_root(lambda k: matrix[k * lines : (k + 1) * lines], matrix[:lines])
    half = exchange(packed_gram(matrix).reshape(2, -1, narrow), "core").sum(axis=0)
    gram_part = exchange(half.reshape(chips, -1, narrow), PLANE).sum(axis=0)
    gram_part = from_root(lambda k: gram_part, gram_part)
    panels = exchange(spread(piece, devices), "col").reshape(-1, WIDE)

    own = exchange(spread(gram_part, chips), PLANE).reshape(-1, narrow)
    inverse = inverse_factor(core, own, swapped(own))

    products = inner(panels, matrix).reshape(2, -1, WIDE)
    mine = jnp.where(core == 0, products[0], products[1])
    half = mine + swapped(jnp.where(core == 0, products[1], products[0]))
    quarter, _ = lax.optimization_barrier((ring_sum(half), own))
    part = exchange(quarter.reshape(lax.axis_size("y"), -1, WIDE), "y").sum(axis=0)
    half = exchange(spread(part, chips), PLANE).reshape(-1, WIDE)
    half, inverse = lax.optimization_barrier((half, inverse))
    first, second = inverse[:, :PANEL], inverse[:, PANEL:]
    there = swapped(half)
    top = product(jnp.where(core == 0, first, second), half)
    top = top + product(jnp.where(core == 0, second, first), there)
    row = lax.broadcasted_iota(jnp.int32, (WIDE, WIDE), 0)
    column = lax.broadcasted_iota(jnp.int32, (WIDE, WIDE), 1)
    top = jnp.where((row > column) & (lax.axis_index("col") == 0), 0.0, top)
    basis = product(panels, inverse.T) * math.sqrt(rows_all)
    return (top, basis)


def solution(mesh):
    finer = Mesh(
        mesh.devices.reshape(4, 8, 2, mesh.shape["col"]), ("x", "y", "core", "col")
    )
    return jax.shard_map(
        body,
        mesh=finer,
        in_specs=(P(ROW, "col"),),
        out_specs=(P(None, "col"), P(ROW, None)),
        check_vma=False,
    )
```

```python
import math

import jax
import jax.numpy as jnp
from jax import lax
from jax.experimental import pallas as pl
from jax.experimental.pallas import tpu as pltpu
from jax.sharding import Mesh
from jax.sharding import PartitionSpec as P


PANEL = 256
WIDE = 2 * PANEL
TILE = 128
STEP = 32
ROW = ("x", "y", "core")
PLANE = ("x", "y")
HIGHEST = lax.Precision.HIGHEST


def inner(left, right):
    return lax.dot_general(
        left,
        right,
        (((0,), (0,)), ((), ())),
        precision=HIGHEST,
        preferred_element_type=jnp.float32,
    )


def product(left, right):
    return jnp.dot(left, right, precision=HIGHEST, preferred_element_type=jnp.float32)


SLOTS = 3
PLACES = {
    (i, j): (n // SLOTS, n % SLOTS)
    for n, (i, j) in enumerate((i, j) for i in range(4) for j in range(i, 4))
}


def blocks_of(place):
    return tuple(slice(p * TILE, (p + 1) * TILE) for p in place)


def gram_kernel(panels_ref, out_ref):
    for i in range(4):
        left = panels_ref[:, i * TILE : (i + 1) * TILE]
        line = inner(left, panels_ref[:, i * TILE :])
        for j in range(i, 4):
            out_ref[blocks_of(PLACES[i, j])] = line[:, (j - i) * TILE : (j - i + 1) * TILE]
    for n in range(len(PLACES), 4 * SLOTS):
        out_ref[blocks_of((n // SLOTS, n % SLOTS))] = jnp.zeros((TILE, TILE), jnp.float32)


def packed_gram(panels):
    vmem = pl.BlockSpec(memory_space=pltpu.VMEM)
    return pl.pallas_call(
        gram_kernel,
        out_shape=jax.ShapeDtypeStruct((WIDE, SLOTS * TILE), jnp.float32),
        in_specs=[vmem],
        out_specs=vmem,
        compiler_params=pltpu.CompilerParams(vmem_limit_bytes=16 * 2**20),
        cost_estimate=pl.CostEstimate(flops=600_000_000, bytes_accessed=2**20, transcendentals=0),
    )(panels)


def factor_kernel(core_ref, own_ref, other_ref, out_ref):
    row8 = lax.broadcasted_iota(jnp.int32, (8, TILE), 0)
    lane = lax.broadcasted_iota(jnp.int32, (8, TILE), 1)
    tiles, groups = WIDE // TILE, STEP // 8
    for half in range(2):

        def take(ref):
            for (i, j), (r, c) in PLACES.items():
                if r // 2 == half:
                    out_ref[blocks_of((i, j))] = ref[blocks_of((r % 2, c))]

        @pl.when(core_ref[0] == half)
        def _():
            take(own_ref)

        @pl.when(core_ref[0] != half)
        def _():
            take(other_ref)

    def outer(t, _):
        base = pl.multiple_of(t * TILE, TILE)
        for u in range(TILE // STEP):
            first = pl.multiple_of(base + u * STEP, STEP)
            block = out_ref[pl.ds(first, STEP), pl.ds(base, TILE)]
            cols = []
            for q in range(STEP):
                spread = jnp.broadcast_to(block[:, u * STEP + q : u * STEP + q + 1], (STEP, TILE))
                cols.append([spread[8 * v : 8 * v + 8] for v in range(groups)])
            rows = []
            for v in range(groups):
                rows.append([])
                for w in range(tiles):
                    values = out_ref[pl.ds(first + 8 * v, 8), TILE * w : TILE * (w + 1)]
                    here = (lane >= u * STEP) & (lane < (u + 1) * STEP) & (t == w)
                    unit = jnp.where(lane - u * STEP == row8 + 8 * v, 1.0, 0.0)
                    rows[v].append(jnp.where(here, unit, values))
            pivots = [None] * groups
            for k in range(STEP):
                vk, sk = k // 8, k % 8
                pivot = jnp.broadcast_to(cols[k][vk][sk : sk + 1], (8, TILE))
                inverse = 1.0 / pivot
                pivots[vk] = pivot if sk == 0 else jnp.where(row8 == sk, pivot, pivots[vk])
                scaled = {}
                for v in range(vk, groups):
                    s = cols[k][v] * inverse
                    scaled[v] = jnp.where(row8 > sk, s, 0.0) if v == vk else s
                for j in range(k + 1, STEP):
                    other = jnp.broadcast_to(cols[k][j // 8][j % 8 : j % 8 + 1], (8, TILE))
                    for v in range(j // 8, groups):
                        cols[j][v] = cols[j][v] - scaled[v] * other
                for w in range(tiles):
                    other = jnp.broadcast_to(rows[vk][w][sk : sk + 1], (8, TILE))
                    for v in range(vk, groups):
                        rows[v][w] = rows[v][w] - scaled[v] * other
            for v in range(groups):
                scale = lax.rsqrt(pivots[v])
                for w in range(tiles):
                    out_ref[pl.ds(first + 8 * v, 8), TILE * w : TILE * (w + 1)] = rows[v][w] * scale
            if u < TILE // STEP - 1:
                rest = TILE - (u + 1) * STEP
                done = out_ref[pl.ds(first, STEP), :]
                left = out_ref[pl.ds(first, STEP), pl.ds(base, TILE)][:, (u + 1) * STEP :]
                old = out_ref[pl.ds(first + STEP, rest), :]
                col = lax.broadcasted_iota(jnp.int32, (rest, WIDE), 1)
                old = jnp.where((col >= first) & (col < first + STEP), 0.0, old)
                out_ref[pl.ds(first + STEP, rest), :] = old - inner(left, done)

        done = out_ref[pl.ds(base, TILE), :]
        row = lax.broadcasted_iota(jnp.int32, (TILE, WIDE), 0) + base
        col = lax.broadcasted_iota(jnp.int32, (TILE, WIDE), 1)
        done = jnp.where((col <= row) | (col >= base + TILE), done, 0.0)

        def below(i, _):
            start = pl.multiple_of(i * TILE, TILE)
            old = out_ref[pl.ds(start, TILE), :]
            old = jnp.where((col >= base) & (col < base + TILE), 0.0, old)
            out_ref[pl.ds(start, TILE), :] = old - inner(
                out_ref[pl.ds(base, TILE), pl.ds(start, TILE)], done
            )
            return 0

        lax.fori_loop(t + 1, tiles, below, 0)
        return 0

    lax.fori_loop(0, tiles, outer, 0)
    row = lax.broadcasted_iota(jnp.int32, (WIDE, WIDE), 0)
    col = lax.broadcasted_iota(jnp.int32, (WIDE, WIDE), 1)
    out_ref[...] = jnp.where(col <= row, out_ref[...], 0.0)


def inverse_factor(core, own, other):
    vmem = pl.BlockSpec(memory_space=pltpu.VMEM)
    return pl.pallas_call(
        factor_kernel,
        out_shape=jax.ShapeDtypeStruct((WIDE, WIDE), jnp.float32),
        in_specs=[pl.BlockSpec(memory_space=pltpu.SMEM), vmem, vmem],
        out_specs=vmem,
        compiler_params=pltpu.CompilerParams(vmem_limit_bytes=16 * 2**20),
        cost_estimate=pl.CostEstimate(
            flops=2_000_000_000, bytes_accessed=2**21, transcendentals=0
        ),
    )(core.reshape(1), own, other)


def exchange(blocks, axis):
    return lax.all_to_all(blocks, axis, 0, 0, tiled=True)


def spread(array, count):
    return jnp.broadcast_to(array[None], (count, *array.shape))


def swapped(array):
    return lax.ppermute(array, "core", [(0, 1), (1, 0)])


def among(index, places):
    found = index == places[0]
    for place in places[1:]:
        found = found | (index == place)
    return found


def steps(matrix):
    rows_all = matrix.shape[0] * lax.axis_size(ROW)
    chips = lax.axis_size(PLANE)
    narrow = SLOTS * TILE
    core = lax.axis_index("core")
    col = lax.axis_index("col")

    far = lax.ppermute(matrix, "col", [(0, 4)])
    packed = packed_gram(matrix)
    half = exchange(packed.reshape(2, -1, narrow), "core").sum(axis=0)
    gram_part = exchange(half.reshape(chips, -1, narrow), PLANE)
    panels = jnp.where(col == 0, matrix, far)
    up = lax.ppermute(panels, "col", [(0, 1), (4, 5)])
    down = lax.ppermute(panels, "col", [(0, 7), (4, 3)])
    gram_part, panels = lax.optimization_barrier((gram_part, panels))
    gram_part = exchange(spread(gram_part.sum(axis=0), lax.axis_size("col")), "col")
    panels = jnp.where(among(col, (1, 5)), up, jnp.where(among(col, (3, 7)), down, panels))
    last = lax.ppermute(panels, "col", [(1, 2), (5, 6)])
    gram_part, panels = lax.optimization_barrier((gram_part, panels))
    own = exchange(spread(gram_part[0], chips), PLANE).reshape(-1, narrow)
    panels = jnp.where(among(col, (2, 6)), last, panels)

    products = inner(panels, matrix).reshape(2, -1, WIDE)
    mine = jnp.where(core == 0, products[0], products[1])
    half = mine + swapped(jnp.where(core == 0, products[1], products[0]))
    half, own = lax.optimization_barrier((half, own))
    part = exchange(half.reshape(chips, -1, WIDE), PLANE)
    inverse = inverse_factor(core, own, swapped(own))
    part, inverse = lax.optimization_barrier((part, inverse))
    half = exchange(spread(part.sum(axis=0), chips), PLANE).reshape(-1, WIDE)
    basis = product(panels, inverse.T) * math.sqrt(rows_all)
    half, basis = lax.optimization_barrier((half, basis))
    first, second = inverse[:, :PANEL], inverse[:, PANEL:]
    there = swapped(half)
    top = product(jnp.where(core == 0, first, second), half)
    top = top + product(jnp.where(core == 0, second, first), there)
    row = lax.broadcasted_iota(jnp.int32, (WIDE, WIDE), 0)
    column = lax.broadcasted_iota(jnp.int32, (WIDE, WIDE), 1)
    top = jnp.where((row > column) & (col == 0), 0.0, top)
    return (top, basis)


def solution(mesh):
    finer = Mesh(
        mesh.devices.reshape(4, 8, 2, mesh.shape["col"]), ("x", "y", "core", "col")
    )
    return jax.shard_map(
        steps,
        mesh=finer,
        in_specs=(P(ROW, "col"),),
        out_specs=(P(None, "col"), P(ROW, None)),
        check_vma=False,
    )
```

```python
import math

import jax
import jax.numpy as jnp
from jax import lax
from jax.experimental import pallas as pl
from jax.experimental.pallas import tpu as pltpu
from jax.sharding import Mesh
from jax.sharding import PartitionSpec as P


PANEL = 256
WIDE = 2 * PANEL
TILE = 128
STEP = 32
ROW = ("x", "y", "core")
PLANE = ("x", "y")
HIGHEST = lax.Precision.HIGHEST


def inner(left, right):
    return lax.dot_general(
        left,
        right,
        (((0,), (0,)), ((), ())),
        precision=HIGHEST,
        preferred_element_type=jnp.float32,
    )


def product(left, right):
    return jnp.dot(left, right, precision=HIGHEST, preferred_element_type=jnp.float32)


SLOTS = 3
PLACES = {
    (i, j): (n // SLOTS, n % SLOTS)
    for n, (i, j) in enumerate((i, j) for i in range(4) for j in range(i, 4))
}


def blocks_of(place):
    return tuple(slice(p * TILE, (p + 1) * TILE) for p in place)


def gram_kernel(panels_ref, out_ref):
    for i in range(4):
        left = panels_ref[:, i * TILE : (i + 1) * TILE]
        line = inner(left, panels_ref[:, i * TILE :])
        for j in range(i, 4):
            out_ref[blocks_of(PLACES[i, j])] = line[:, (j - i) * TILE : (j - i + 1) * TILE]
    for n in range(len(PLACES), 4 * SLOTS):
        out_ref[blocks_of((n // SLOTS, n % SLOTS))] = jnp.zeros((TILE, TILE), jnp.float32)


def start_kernel(core_ref, own_ref, other_ref, out_ref):
    for half in range(2):

        def take(ref):
            for (i, j), (r, c) in PLACES.items():
                if r // 2 == half:
                    out_ref[blocks_of((i, j))] = ref[blocks_of((r % 2, c))]

        @pl.when(core_ref[0] == half)
        def _():
            take(own_ref)

        @pl.when(core_ref[0] != half)
        def _():
            take(other_ref)

    factor_tiles(out_ref, 0, 2)


def finish_kernel(state_ref, out_ref):
    out_ref[...] = state_ref[...]
    factor_tiles(out_ref, 2, 4)
    row = lax.broadcasted_iota(jnp.int32, (WIDE, WIDE), 0)
    col = lax.broadcasted_iota(jnp.int32, (WIDE, WIDE), 1)
    out_ref[...] = jnp.where(col <= row, out_ref[...], 0.0)


def factor_tiles(out_ref, begin, end):
    row8 = lax.broadcasted_iota(jnp.int32, (8, TILE), 0)
    lane = lax.broadcasted_iota(jnp.int32, (8, TILE), 1)
    tiles, groups = WIDE // TILE, STEP // 8

    def outer(t, _):
        base = pl.multiple_of(t * TILE, TILE)
        for u in range(TILE // STEP):
            first = pl.multiple_of(base + u * STEP, STEP)
            block = out_ref[pl.ds(first, STEP), pl.ds(base, TILE)]
            cols = []
            for q in range(STEP):
                spread = jnp.broadcast_to(block[:, u * STEP + q : u * STEP + q + 1], (STEP, TILE))
                cols.append([spread[8 * v : 8 * v + 8] for v in range(groups)])
            rows = []
            for v in range(groups):
                rows.append([])
                for w in range(tiles):
                    values = out_ref[pl.ds(first + 8 * v, 8), TILE * w : TILE * (w + 1)]
                    here = (lane >= u * STEP) & (lane < (u + 1) * STEP) & (t == w)
                    unit = jnp.where(lane - u * STEP == row8 + 8 * v, 1.0, 0.0)
                    rows[v].append(jnp.where(here, unit, values))
            pivots = [None] * groups
            for k in range(STEP):
                vk, sk = k // 8, k % 8
                pivot = jnp.broadcast_to(cols[k][vk][sk : sk + 1], (8, TILE))
                inverse = 1.0 / pivot
                pivots[vk] = pivot if sk == 0 else jnp.where(row8 == sk, pivot, pivots[vk])
                scaled = {}
                for v in range(vk, groups):
                    s = cols[k][v] * inverse
                    scaled[v] = jnp.where(row8 > sk, s, 0.0) if v == vk else s
                for j in range(k + 1, STEP):
                    other = jnp.broadcast_to(cols[k][j // 8][j % 8 : j % 8 + 1], (8, TILE))
                    for v in range(j // 8, groups):
                        cols[j][v] = cols[j][v] - scaled[v] * other
                for w in range(tiles):
                    other = jnp.broadcast_to(rows[vk][w][sk : sk + 1], (8, TILE))
                    for v in range(vk, groups):
                        rows[v][w] = rows[v][w] - scaled[v] * other
            for v in range(groups):
                scale = lax.rsqrt(pivots[v])
                for w in range(tiles):
                    out_ref[pl.ds(first + 8 * v, 8), TILE * w : TILE * (w + 1)] = rows[v][w] * scale
            if u < TILE // STEP - 1:
                rest = TILE - (u + 1) * STEP
                done = out_ref[pl.ds(first, STEP), :]
                left = out_ref[pl.ds(first, STEP), pl.ds(base, TILE)][:, (u + 1) * STEP :]
                old = out_ref[pl.ds(first + STEP, rest), :]
                col = lax.broadcasted_iota(jnp.int32, (rest, WIDE), 1)
                old = jnp.where((col >= first) & (col < first + STEP), 0.0, old)
                out_ref[pl.ds(first + STEP, rest), :] = old - inner(left, done)

        done = out_ref[pl.ds(base, TILE), :]
        row = lax.broadcasted_iota(jnp.int32, (TILE, WIDE), 0) + base
        col = lax.broadcasted_iota(jnp.int32, (TILE, WIDE), 1)
        done = jnp.where((col <= row) | (col >= base + TILE), done, 0.0)

        def below(i, _):
            start = pl.multiple_of(i * TILE, TILE)
            old = out_ref[pl.ds(start, TILE), :]
            old = jnp.where((col >= base) & (col < base + TILE), 0.0, old)
            out_ref[pl.ds(start, TILE), :] = old - inner(
                out_ref[pl.ds(base, TILE), pl.ds(start, TILE)], done
            )
            return 0

        lax.fori_loop(t + 1, tiles, below, 0)
        return 0

    lax.fori_loop(begin, end, outer, 0)


def call(kernel, operands, rows, columns, flops):
    vmem, smem = pl.BlockSpec(memory_space=pltpu.VMEM), pl.BlockSpec(memory_space=pltpu.SMEM)
    return pl.pallas_call(
        kernel,
        out_shape=jax.ShapeDtypeStruct((rows, columns), jnp.float32),
        in_specs=[smem if a.ndim == 1 else vmem for a in operands],
        out_specs=vmem,
        compiler_params=pltpu.CompilerParams(vmem_limit_bytes=16 * 2**20),
        cost_estimate=pl.CostEstimate(flops=flops, bytes_accessed=2**21, transcendentals=0),
    )(*operands)


def exchange(blocks, axis):
    return lax.all_to_all(blocks, axis, 0, 0, tiled=True)


def spread(array, count):
    return jnp.broadcast_to(array[None], (count, *array.shape))


def swapped(array):
    return lax.ppermute(array, "core", [(0, 1), (1, 0)])


def steps(matrix):
    rows_all = matrix.shape[0] * lax.axis_size(ROW)
    chips = lax.axis_size(PLANE)
    narrow = SLOTS * TILE
    core = lax.axis_index("core")
    col = lax.axis_index("col")

    up = lax.ppermute(matrix, "col", [(0, 3)])
    down = lax.ppermute(matrix, "col", [(0, 5)])
    packed = call(gram_kernel, (matrix,), WIDE, narrow, 600_000_000)
    half = exchange(packed.reshape(2, -1, narrow), "core").sum(axis=0)
    gram_part = exchange(half.reshape(chips, -1, narrow), PLANE)
    panels = jnp.where(col == 0, matrix, up + down)
    up = lax.ppermute(panels, "col", [(0, 1), (3, 4), (5, 6)])
    down = lax.ppermute(panels, "col", [(0, 7), (3, 2)])
    gram_part, panels = lax.optimization_barrier((gram_part, panels))
    gram_part = exchange(spread(gram_part.sum(axis=0), lax.axis_size("col")), "col")
    own = exchange(spread(gram_part[0], chips), PLANE).reshape(-1, narrow)
    panels = jnp.where((col == 0) | (col == 3) | (col == 5), panels, up + down)
    products = inner(panels, matrix).reshape(2, -1, WIDE)
    mine = jnp.where(core == 0, products[0], products[1])
    half = mine + swapped(jnp.where(core == 0, products[1], products[0]))
    half, own = lax.optimization_barrier((half, own))
    part = exchange(half.reshape(chips, -1, WIDE), PLANE)
    state = call(start_kernel, (core.reshape(1), own, swapped(own)), WIDE, WIDE, 1_000_000_000)
    part, state = lax.optimization_barrier((part, state))
    half = exchange(spread(part.sum(axis=0), chips), PLANE).reshape(-1, WIDE)
    inverse = call(finish_kernel, (state,), WIDE, WIDE, 1_000_000_000)
    basis = product(panels, inverse.T) * math.sqrt(rows_all)
    half, basis = lax.optimization_barrier((half, basis))
    first, second = inverse[:, :PANEL], inverse[:, PANEL:]
    there = swapped(half)
    top = product(jnp.where(core == 0, first, second), half)
    top = top + product(jnp.where(core == 0, second, first), there)
    row = lax.broadcasted_iota(jnp.int32, (WIDE, WIDE), 0)
    column = lax.broadcasted_iota(jnp.int32, (WIDE, WIDE), 1)
    top = jnp.where((row > column) & (col == 0), 0.0, top)
    return (top, basis)


def solution(mesh):
    finer = Mesh(
        mesh.devices.reshape(4, 8, 2, mesh.shape["col"]), ("x", "y", "core", "col")
    )
    return jax.shard_map(
        steps,
        mesh=finer,
        in_specs=(P(ROW, "col"),),
        out_specs=(P(None, "col"), P(ROW, None)),
        check_vma=False,
    )
```

```python
import math

import jax
import jax.numpy as jnp
from jax import lax
from jax.experimental import pallas as pl
from jax.experimental.pallas import tpu as pltpu
from jax.sharding import Mesh
from jax.sharding import PartitionSpec as P


PANEL = 256
WIDE = 2 * PANEL
TILE = 128
STEP = 32
ROW = ("x", "y", "core")
PLANE = ("x", "y")
HIGHEST = lax.Precision.HIGHEST


def inner(left, right):
    return lax.dot_general(
        left,
        right,
        (((0,), (0,)), ((), ())),
        precision=HIGHEST,
        preferred_element_type=jnp.float32,
    )


def product(left, right):
    return jnp.dot(left, right, precision=HIGHEST, preferred_element_type=jnp.float32)


SLOTS = 3
PLACES = {
    (i, j): (n // SLOTS, n % SLOTS)
    for n, (i, j) in enumerate((i, j) for i in range(4) for j in range(i, 4))
}


def blocks_of(place):
    return tuple(slice(p * TILE, (p + 1) * TILE) for p in place)


def gram_kernel(panels_ref, out_ref):
    for i in range(4):
        left = panels_ref[:, i * TILE : (i + 1) * TILE]
        line = inner(left, panels_ref[:, i * TILE :])
        for j in range(i, 4):
            out_ref[blocks_of(PLACES[i, j])] = line[:, (j - i) * TILE : (j - i + 1) * TILE]
    for n in range(len(PLACES), 4 * SLOTS):
        out_ref[blocks_of((n // SLOTS, n % SLOTS))] = jnp.zeros((TILE, TILE), jnp.float32)


def start_kernel(core_ref, own_ref, other_ref, out_ref):
    for half in range(2):

        def take(ref):
            for (i, j), (r, c) in PLACES.items():
                if r // 2 == half:
                    out_ref[blocks_of((i, j))] = ref[blocks_of((r % 2, c))]

        @pl.when(core_ref[0] == half)
        def _():
            take(own_ref)

        @pl.when(core_ref[0] != half)
        def _():
            take(other_ref)

    factor_tiles(out_ref, 0, 1)


def finish_kernel(state_ref, out_ref):
    out_ref[...] = state_ref[...]
    factor_tiles(out_ref, 1, 4)
    row = lax.broadcasted_iota(jnp.int32, (WIDE, WIDE), 0)
    col = lax.broadcasted_iota(jnp.int32, (WIDE, WIDE), 1)
    out_ref[...] = jnp.where(col <= row, out_ref[...], 0.0)


def factor_tiles(out_ref, begin, end):
    row8 = lax.broadcasted_iota(jnp.int32, (8, TILE), 0)
    lane = lax.broadcasted_iota(jnp.int32, (8, TILE), 1)
    tiles, groups = WIDE // TILE, STEP // 8

    def outer(t, _):
        base = pl.multiple_of(t * TILE, TILE)
        for u in range(TILE // STEP):
            first = pl.multiple_of(base + u * STEP, STEP)
            block = out_ref[pl.ds(first, STEP), pl.ds(base, TILE)]
            cols = []
            for q in range(STEP):
                spread = jnp.broadcast_to(block[:, u * STEP + q : u * STEP + q + 1], (STEP, TILE))
                cols.append([spread[8 * v : 8 * v + 8] for v in range(groups)])
            rows = []
            for v in range(groups):
                rows.append([])
                for w in range(tiles):
                    values = out_ref[pl.ds(first + 8 * v, 8), TILE * w : TILE * (w + 1)]
                    here = (lane >= u * STEP) & (lane < (u + 1) * STEP) & (t == w)
                    unit = jnp.where(lane - u * STEP == row8 + 8 * v, 1.0, 0.0)
                    rows[v].append(jnp.where(here, unit, values))
            pivots = [None] * groups
            for k in range(STEP):
                vk, sk = k // 8, k % 8
                pivot = jnp.broadcast_to(cols[k][vk][sk : sk + 1], (8, TILE))
                inverse = 1.0 / pivot
                pivots[vk] = pivot if sk == 0 else jnp.where(row8 == sk, pivot, pivots[vk])
                scaled = {}
                for v in range(vk, groups):
                    s = cols[k][v] * inverse
                    scaled[v] = jnp.where(row8 > sk, s, 0.0) if v == vk else s
                for j in range(k + 1, STEP):
                    other = jnp.broadcast_to(cols[k][j // 8][j % 8 : j % 8 + 1], (8, TILE))
                    for v in range(j // 8, groups):
                        cols[j][v] = cols[j][v] - scaled[v] * other
                for w in range(tiles):
                    other = jnp.broadcast_to(rows[vk][w][sk : sk + 1], (8, TILE))
                    for v in range(vk, groups):
                        rows[v][w] = rows[v][w] - scaled[v] * other
            for v in range(groups):
                scale = lax.rsqrt(pivots[v])
                for w in range(tiles):
                    out_ref[pl.ds(first + 8 * v, 8), TILE * w : TILE * (w + 1)] = rows[v][w] * scale
            if u < TILE // STEP - 1:
                rest = TILE - (u + 1) * STEP
                done = out_ref[pl.ds(first, STEP), :]
                left = out_ref[pl.ds(first, STEP), pl.ds(base, TILE)][:, (u + 1) * STEP :]
                old = out_ref[pl.ds(first + STEP, rest), :]
                col = lax.broadcasted_iota(jnp.int32, (rest, WIDE), 1)
                old = jnp.where((col >= first) & (col < first + STEP), 0.0, old)
                out_ref[pl.ds(first + STEP, rest), :] = old - inner(left, done)

        done = out_ref[pl.ds(base, TILE), :]
        row = lax.broadcasted_iota(jnp.int32, (TILE, WIDE), 0) + base
        col = lax.broadcasted_iota(jnp.int32, (TILE, WIDE), 1)
        done = jnp.where((col <= row) | (col >= base + TILE), done, 0.0)

        def below(i, _):
            start = pl.multiple_of(i * TILE, TILE)
            old = out_ref[pl.ds(start, TILE), :]
            old = jnp.where((col >= base) & (col < base + TILE), 0.0, old)
            out_ref[pl.ds(start, TILE), :] = old - inner(
                out_ref[pl.ds(base, TILE), pl.ds(start, TILE)], done
            )
            return 0

        lax.fori_loop(t + 1, tiles, below, 0)
        return 0

    lax.fori_loop(begin, end, outer, 0)


def call(kernel, operands, rows, columns, flops):
    vmem, smem = pl.BlockSpec(memory_space=pltpu.VMEM), pl.BlockSpec(memory_space=pltpu.SMEM)
    return pl.pallas_call(
        kernel,
        out_shape=jax.ShapeDtypeStruct((rows, columns), jnp.float32),
        in_specs=[smem if a.ndim == 1 else vmem for a in operands],
        out_specs=vmem,
        compiler_params=pltpu.CompilerParams(vmem_limit_bytes=16 * 2**20),
        cost_estimate=pl.CostEstimate(flops=flops, bytes_accessed=2**21, transcendentals=0),
    )(*operands)


def exchange(blocks, axis):
    return lax.all_to_all(blocks, axis, 0, 0, tiled=True)


def spread(array, count):
    return jnp.broadcast_to(array[None], (count, *array.shape))


def swapped(array):
    return lax.ppermute(array, "core", [(0, 1), (1, 0)])


def steps(matrix):
    rows_all = matrix.shape[0] * lax.axis_size(ROW)
    chips = lax.axis_size(PLANE)
    narrow = SLOTS * TILE
    core = lax.axis_index("core")
    col = lax.axis_index("col")

    up = lax.ppermute(matrix, "col", [(0, 3)])
    down = lax.ppermute(matrix, "col", [(0, 5)])
    packed = call(gram_kernel, (matrix,), WIDE, narrow, 600_000_000)
    half = exchange(packed.reshape(2, -1, narrow), "core").sum(axis=0)
    gram_part = exchange(half.reshape(chips, -1, narrow), PLANE)
    panels = jnp.where(col == 0, matrix, up + down)
    up = lax.ppermute(panels, "col", [(0, 1), (3, 4), (5, 6)])
    down = lax.ppermute(panels, "col", [(0, 7), (3, 2)])
    gram_part = exchange(spread(gram_part.sum(axis=0), lax.axis_size("col")), "col")
    own = exchange(spread(gram_part[0], chips), PLANE).reshape(-1, narrow)
    panels = jnp.where((col == 0) | (col == 3) | (col == 5), panels, up + down)
    panels = lax.optimization_barrier(panels)
    products = inner(panels, matrix).reshape(2, -1, WIDE)
    mine = jnp.where(core == 0, products[0], products[1])
    half = mine + swapped(jnp.where(core == 0, products[1], products[0]))
    half, own = lax.optimization_barrier((half, own))
    part = exchange(half.reshape(chips, -1, WIDE), PLANE)
    state = call(start_kernel, (core.reshape(1), own, swapped(own)), WIDE, WIDE, 1_000_000_000)
    part, state = lax.optimization_barrier((part, state))
    half = exchange(spread(part.sum(axis=0), chips), PLANE).reshape(-1, WIDE)
    inverse = call(finish_kernel, (state,), WIDE, WIDE, 1_000_000_000)
    basis = product(panels, inverse.T) * math.sqrt(rows_all)
    half, basis = lax.optimization_barrier((half, basis))
    first, second = inverse[:, :PANEL], inverse[:, PANEL:]
    there = swapped(half)
    top = product(jnp.where(core == 0, first, second), half)
    top = top + product(jnp.where(core == 0, second, first), there)
    row = lax.broadcasted_iota(jnp.int32, (WIDE, WIDE), 0)
    column = lax.broadcasted_iota(jnp.int32, (WIDE, WIDE), 1)
    top = jnp.where((row > column) & (col == 0), 0.0, top)
    return (top, basis)


def solution(mesh):
    finer = Mesh(
        mesh.devices.reshape(4, 8, 2, mesh.shape["col"]), ("x", "y", "core", "col")
    )
    return jax.shard_map(
        steps,
        mesh=finer,
        in_specs=(P(ROW, "col"),),
        out_specs=(P(None, "col"), P(ROW, None)),
        check_vma=False,
    )
```

```python
import math

import jax
import jax.numpy as jnp
from jax import lax
from jax.experimental import pallas as pl
from jax.experimental.pallas import tpu as pltpu
from jax.sharding import Mesh
from jax.sharding import PartitionSpec as P


PANEL = 256
WIDE = 2 * PANEL
TILE = 128
STEP = 32
ROW = ("x", "y", "core")
PLANE = ("x", "y")
HIGHEST = lax.Precision.HIGHEST


def inner(left, right):
    return lax.dot_general(
        left,
        right,
        (((0,), (0,)), ((), ())),
        precision=HIGHEST,
        preferred_element_type=jnp.float32,
    )


def product(left, right):
    return jnp.dot(left, right, precision=HIGHEST, preferred_element_type=jnp.float32)


PLACES = {
    (0, 0): (0, 0), (0, 1): (0, 1), (0, 2): (0, 2), (0, 3): (0, 3), (3, 3): (0, 4),
    (1, 1): (1, 0), (1, 2): (1, 1), (1, 3): (1, 2), (2, 2): (1, 3), (2, 3): (1, 4),
}
NARROW = 5 * TILE


def span(place):
    return slice(place * TILE, (place + 1) * TILE)


def gram_kernel(core_ref, panels_ref, keep_ref, send_ref):
    for i in range(4):
        line = inner(panels_ref[:, span(i)], panels_ref[:, i * TILE :])
        half = PLACES[i, i][0]

        def put(ref):
            for j in range(i, 4):
                block = line[:, span(j - i)]
                ref[:, :, span(PLACES[i, j][1])] = block.reshape(*ref.shape[:2], TILE)

        @pl.when(core_ref[0] == half)
        def _():
            put(keep_ref)

        @pl.when(core_ref[0] != half)
        def _():
            put(send_ref)


def start_kernel(core_ref, own_ref, other_ref, out_ref):
    for half in range(2):

        def take(ref):
            for (i, j), (where, place) in PLACES.items():
                if where == half:
                    out_ref[span(i), span(j)] = ref[:, :, span(place)].reshape(TILE, TILE)

        @pl.when(core_ref[0] == half)
        def _():
            take(own_ref)

        @pl.when(core_ref[0] != half)
        def _():
            take(other_ref)

    factor_tiles(out_ref, 0, 1)


def finish_kernel(state_ref, out_ref):
    out_ref[...] = state_ref[...]
    factor_tiles(out_ref, 1, 4)
    row = lax.broadcasted_iota(jnp.int32, (WIDE, WIDE), 0)
    col = lax.broadcasted_iota(jnp.int32, (WIDE, WIDE), 1)
    out_ref[...] = jnp.where(col <= row, out_ref[...], 0.0)


def factor_tiles(out_ref, begin, end):
    row8 = lax.broadcasted_iota(jnp.int32, (8, TILE), 0)
    lane = lax.broadcasted_iota(jnp.int32, (8, TILE), 1)
    tiles, groups = WIDE // TILE, STEP // 8

    def outer(t, _):
        base = pl.multiple_of(t * TILE, TILE)
        for u in range(TILE // STEP):
            first = pl.multiple_of(base + u * STEP, STEP)
            block = out_ref[pl.ds(first, STEP), pl.ds(base, TILE)]
            cols = []
            for q in range(STEP):
                spread = jnp.broadcast_to(block[:, u * STEP + q : u * STEP + q + 1], (STEP, TILE))
                cols.append([spread[8 * v : 8 * v + 8] for v in range(groups)])
            rows = []
            for v in range(groups):
                rows.append([])
                for w in range(tiles):
                    values = out_ref[pl.ds(first + 8 * v, 8), TILE * w : TILE * (w + 1)]
                    here = (lane >= u * STEP) & (lane < (u + 1) * STEP) & (t == w)
                    unit = jnp.where(lane - u * STEP == row8 + 8 * v, 1.0, 0.0)
                    rows[v].append(jnp.where(here, unit, values))
            pivots = [None] * groups
            for k in range(STEP):
                vk, sk = k // 8, k % 8
                pivot = jnp.broadcast_to(cols[k][vk][sk : sk + 1], (8, TILE))
                inverse = 1.0 / pivot
                pivots[vk] = pivot if sk == 0 else jnp.where(row8 == sk, pivot, pivots[vk])
                scaled = {}
                for v in range(vk, groups):
                    s = cols[k][v] * inverse
                    scaled[v] = jnp.where(row8 > sk, s, 0.0) if v == vk else s
                for j in range(k + 1, STEP):
                    other = jnp.broadcast_to(cols[k][j // 8][j % 8 : j % 8 + 1], (8, TILE))
                    for v in range(j // 8, groups):
                        cols[j][v] = cols[j][v] - scaled[v] * other
                for w in range(tiles):
                    other = jnp.broadcast_to(rows[vk][w][sk : sk + 1], (8, TILE))
                    for v in range(vk, groups):
                        rows[v][w] = rows[v][w] - scaled[v] * other
            for v in range(groups):
                scale = lax.rsqrt(pivots[v])
                for w in range(tiles):
                    out_ref[pl.ds(first + 8 * v, 8), TILE * w : TILE * (w + 1)] = rows[v][w] * scale
            if u < TILE // STEP - 1:
                rest = TILE - (u + 1) * STEP
                done = out_ref[pl.ds(first, STEP), :]
                left = out_ref[pl.ds(first, STEP), pl.ds(base, TILE)][:, (u + 1) * STEP :]
                old = out_ref[pl.ds(first + STEP, rest), :]
                col = lax.broadcasted_iota(jnp.int32, (rest, WIDE), 1)
                old = jnp.where((col >= first) & (col < first + STEP), 0.0, old)
                out_ref[pl.ds(first + STEP, rest), :] = old - inner(left, done)

        done = out_ref[pl.ds(base, TILE), :]
        row = lax.broadcasted_iota(jnp.int32, (TILE, WIDE), 0) + base
        col = lax.broadcasted_iota(jnp.int32, (TILE, WIDE), 1)
        done = jnp.where((col <= row) | (col >= base + TILE), done, 0.0)

        def below(i, _):
            start = pl.multiple_of(i * TILE, TILE)
            old = out_ref[pl.ds(start, TILE), :]
            old = jnp.where((col >= base) & (col < base + TILE), 0.0, old)
            out_ref[pl.ds(start, TILE), :] = old - inner(
                out_ref[pl.ds(base, TILE), pl.ds(start, TILE)], done
            )
            return 0

        lax.fori_loop(t + 1, tiles, below, 0)
        return 0

    lax.fori_loop(begin, end, outer, 0)


def call(kernel, operands, shapes, flops):
    vmem, smem = pl.BlockSpec(memory_space=pltpu.VMEM), pl.BlockSpec(memory_space=pltpu.SMEM)
    return pl.pallas_call(
        kernel,
        out_shape=[jax.ShapeDtypeStruct(shape, jnp.float32) for shape in shapes],
        in_specs=[smem if a.ndim == 1 else vmem for a in operands],
        out_specs=[vmem for _ in shapes],
        compiler_params=pltpu.CompilerParams(vmem_limit_bytes=16 * 2**20),
        cost_estimate=pl.CostEstimate(flops=flops, bytes_accessed=2**21, transcendentals=0),
    )(*operands)


def exchange(blocks, axis):
    return lax.all_to_all(blocks, axis, 0, 0, tiled=True)


def spread(array, count):
    return jnp.broadcast_to(array[None], (count, *array.shape))


def swapped(array):
    return lax.ppermute(array, "core", [(0, 1), (1, 0)])


def steps(matrix):
    rows_all = matrix.shape[0] * lax.axis_size(ROW)
    chips = lax.axis_size(PLANE)
    core = lax.axis_index("core")
    which = core.reshape(1)
    col = lax.axis_index("col")

    up = lax.ppermute(matrix, "col", [(0, 3)])
    down = lax.ppermute(matrix, "col", [(0, 5)])
    keep, send = call(gram_kernel, (which, matrix), [(chips, TILE // chips, NARROW)] * 2, 600_000_000)
    half = keep + swapped(send)
    gram_part = exchange(half, PLANE)
    panels = jnp.where(col == 0, matrix, up + down)
    up = lax.ppermute(panels, "col", [(0, 1), (3, 4), (5, 6)])
    down = lax.ppermute(panels, "col", [(0, 7), (3, 2)])
    gram_part = gram_part.sum(axis=0)
    copies = [
        lax.ppermute(gram_part, "col", [(0, k)]) for k in range(1, lax.axis_size("col"))
    ]
    gram_part = jnp.where(col == 0, gram_part, sum(copies))
    own = exchange(spread(gram_part, chips), PLANE)
    panels = jnp.where((col == 0) | (col == 3) | (col == 5), panels, up + down)
    panels = lax.optimization_barrier(panels)
    products = inner(panels, matrix).reshape(2, -1, WIDE)
    mine = jnp.where(core == 0, products[0], products[1])
    half = mine + swapped(jnp.where(core == 0, products[1], products[0]))
    half, own = lax.optimization_barrier((half, own))
    part = exchange(half.reshape(chips, -1, WIDE), PLANE)
    (state,) = call(start_kernel, (which, own, swapped(own)), [(WIDE, WIDE)], 1_000_000_000)
    part, state = lax.optimization_barrier((part, state))
    half = exchange(spread(part.sum(axis=0), chips), PLANE).reshape(-1, WIDE)
    (inverse,) = call(finish_kernel, (state,), [(WIDE, WIDE)], 1_000_000_000)
    basis = product(panels, inverse.T) * math.sqrt(rows_all)
    half, basis = lax.optimization_barrier((half, basis))
    first, second = inverse[:, :PANEL], inverse[:, PANEL:]
    there = swapped(half)
    top = product(jnp.where(core == 0, first, second), half)
    top = top + product(jnp.where(core == 0, second, first), there)
    row = lax.broadcasted_iota(jnp.int32, (WIDE, WIDE), 0)
    column = lax.broadcasted_iota(jnp.int32, (WIDE, WIDE), 1)
    top = jnp.where((row > column) & (col == 0), 0.0, top)
    return (top, basis)


def solution(mesh):
    finer = Mesh(
        mesh.devices.reshape(4, 8, 2, mesh.shape["col"]), ("x", "y", "core", "col")
    )
    return jax.shard_map(
        steps,
        mesh=finer,
        in_specs=(P(ROW, "col"),),
        out_specs=(P(None, "col"), P(ROW, None)),
        check_vma=False,
    )
```

```python
import math

import jax
import jax.numpy as jnp
from jax import lax
from jax.experimental import pallas as pl
from jax.experimental.pallas import tpu as pltpu
from jax.sharding import Mesh
from jax.sharding import PartitionSpec as P


PANEL = 256
WIDE = 2 * PANEL
TILE = 128
STEP = 32
ROW = ("x", "y", "core")
PLANE = ("x", "y")
HIGHEST = lax.Precision.HIGHEST


def inner(left, right):
    return lax.dot_general(
        left,
        right,
        (((0,), (0,)), ((), ())),
        precision=HIGHEST,
        preferred_element_type=jnp.float32,
    )


def product(left, right):
    return jnp.dot(left, right, precision=HIGHEST, preferred_element_type=jnp.float32)


PLACES = {
    (0, 0): (0, 0), (0, 1): (0, 1), (0, 2): (0, 2), (0, 3): (0, 3), (3, 3): (0, 4),
    (1, 1): (1, 0), (1, 2): (1, 1), (1, 3): (1, 2), (2, 2): (1, 3), (2, 3): (1, 4),
}
NARROW = 5 * TILE


def span(place):
    return slice(place * TILE, (place + 1) * TILE)


def gram_kernel(core_ref, panels_ref, keep_ref, send_ref):
    for i in range(4):
        line = inner(panels_ref[:, span(i)], panels_ref[:, i * TILE :])
        half = PLACES[i, i][0]

        def put(ref):
            for j in range(i, 4):
                block = line[:, span(j - i)]
                ref[:, :, span(PLACES[i, j][1])] = block.reshape(*ref.shape[:2], TILE)

        @pl.when(core_ref[0] == half)
        def _():
            put(keep_ref)

        @pl.when(core_ref[0] != half)
        def _():
            put(send_ref)


def start_kernel(core_ref, own_ref, other_ref, out_ref):
    for half in range(2):

        def take(ref):
            for (i, j), (where, place) in PLACES.items():
                if where == half:
                    out_ref[span(i), span(j)] = ref[:, :, span(place)].reshape(TILE, TILE)

        @pl.when(core_ref[0] == half)
        def _():
            take(own_ref)

        @pl.when(core_ref[0] != half)
        def _():
            take(other_ref)

    factor_tiles(out_ref, 0, 1)


def finish_kernel(state_ref, out_ref):
    out_ref[...] = state_ref[...]
    factor_tiles(out_ref, 1, 4)
    row = lax.broadcasted_iota(jnp.int32, (WIDE, WIDE), 0)
    col = lax.broadcasted_iota(jnp.int32, (WIDE, WIDE), 1)
    out_ref[...] = jnp.where(col <= row, out_ref[...], 0.0)


def factor_tiles(out_ref, begin, end):
    row8 = lax.broadcasted_iota(jnp.int32, (8, TILE), 0)
    lane = lax.broadcasted_iota(jnp.int32, (8, TILE), 1)
    tiles, groups = WIDE // TILE, STEP // 8

    def outer(t, _):
        base = pl.multiple_of(t * TILE, TILE)
        for u in range(TILE // STEP):
            first = pl.multiple_of(base + u * STEP, STEP)
            block = out_ref[pl.ds(first, STEP), pl.ds(base, TILE)]
            cols = []
            for q in range(STEP):
                spread = jnp.broadcast_to(block[:, u * STEP + q : u * STEP + q + 1], (STEP, TILE))
                cols.append([spread[8 * v : 8 * v + 8] for v in range(groups)])
            rows = []
            for v in range(groups):
                rows.append([])
                for w in range(tiles):
                    values = out_ref[pl.ds(first + 8 * v, 8), TILE * w : TILE * (w + 1)]
                    here = (lane >= u * STEP) & (lane < (u + 1) * STEP) & (t == w)
                    unit = jnp.where(lane - u * STEP == row8 + 8 * v, 1.0, 0.0)
                    rows[v].append(jnp.where(here, unit, values))
            pivots = [None] * groups
            for k in range(STEP):
                vk, sk = k // 8, k % 8
                pivot = jnp.broadcast_to(cols[k][vk][sk : sk + 1], (8, TILE))
                inverse = 1.0 / pivot
                pivots[vk] = pivot if sk == 0 else jnp.where(row8 == sk, pivot, pivots[vk])
                scaled = {}
                for v in range(vk, groups):
                    s = cols[k][v] * inverse
                    scaled[v] = jnp.where(row8 > sk, s, 0.0) if v == vk else s
                for j in range(k + 1, STEP):
                    other = jnp.broadcast_to(cols[k][j // 8][j % 8 : j % 8 + 1], (8, TILE))
                    for v in range(j // 8, groups):
                        cols[j][v] = cols[j][v] - scaled[v] * other
                for w in range(tiles):
                    other = jnp.broadcast_to(rows[vk][w][sk : sk + 1], (8, TILE))
                    for v in range(vk, groups):
                        rows[v][w] = rows[v][w] - scaled[v] * other
            for v in range(groups):
                scale = lax.rsqrt(pivots[v])
                for w in range(tiles):
                    out_ref[pl.ds(first + 8 * v, 8), TILE * w : TILE * (w + 1)] = rows[v][w] * scale
            if u < TILE // STEP - 1:
                rest = TILE - (u + 1) * STEP
                done = out_ref[pl.ds(first, STEP), :]
                left = out_ref[pl.ds(first, STEP), pl.ds(base, TILE)][:, (u + 1) * STEP :]
                old = out_ref[pl.ds(first + STEP, rest), :]
                col = lax.broadcasted_iota(jnp.int32, (rest, WIDE), 1)
                old = jnp.where((col >= first) & (col < first + STEP), 0.0, old)
                out_ref[pl.ds(first + STEP, rest), :] = old - inner(left, done)

        done = out_ref[pl.ds(base, TILE), :]
        row = lax.broadcasted_iota(jnp.int32, (TILE, WIDE), 0) + base
        col = lax.broadcasted_iota(jnp.int32, (TILE, WIDE), 1)
        done = jnp.where((col <= row) | (col >= base + TILE), done, 0.0)

        def below(i, _):
            start = pl.multiple_of(i * TILE, TILE)
            old = out_ref[pl.ds(start, TILE), :]
            old = jnp.where((col >= base) & (col < base + TILE), 0.0, old)
            out_ref[pl.ds(start, TILE), :] = old - inner(
                out_ref[pl.ds(base, TILE), pl.ds(start, TILE)], done
            )
            return 0

        lax.fori_loop(t + 1, tiles, below, 0)
        return 0

    lax.fori_loop(begin, end, outer, 0)


def call(kernel, operands, shapes, flops):
    vmem, smem = pl.BlockSpec(memory_space=pltpu.VMEM), pl.BlockSpec(memory_space=pltpu.SMEM)
    return pl.pallas_call(
        kernel,
        out_shape=[jax.ShapeDtypeStruct(shape, jnp.float32) for shape in shapes],
        in_specs=[smem if a.ndim == 1 else vmem for a in operands],
        out_specs=[vmem for _ in shapes],
        compiler_params=pltpu.CompilerParams(vmem_limit_bytes=16 * 2**20),
        cost_estimate=pl.CostEstimate(flops=flops, bytes_accessed=2**21, transcendentals=0),
    )(*operands)


def exchange(blocks, axis):
    return lax.all_to_all(blocks, axis, 0, 0, tiled=True)


def spread(array, count):
    return jnp.broadcast_to(array[None], (count, *array.shape))


def swapped(array):
    return lax.ppermute(array, "core", [(0, 1), (1, 0)])


def gathered_along_x(array):
    count = lax.axis_size("x")
    pieces = [array]
    for step in range(1, count):
        pairs = [(i, (i + step) % count) for i in range(count)]
        pieces.append(lax.ppermute(array, "x", pairs))
    lines = []
    for place in range(count):
        line = pieces[0]
        for step in range(1, count):
            source = lax.rem(lax.axis_index("x") + count - step, count)
            line = jnp.where(source == place, pieces[step], line)
        lines.append(line)
    return jnp.concatenate(lines)


def steps(matrix):
    rows_all = matrix.shape[0] * lax.axis_size(ROW)
    chips = lax.axis_size(PLANE)
    core = lax.axis_index("core")
    which = core.reshape(1)
    col = lax.axis_index("col")

    up = lax.ppermute(matrix, "col", [(0, 3)])
    down = lax.ppermute(matrix, "col", [(0, 5)])
    keep, send = call(gram_kernel, (which, matrix), [(chips, TILE // chips, NARROW)] * 2, 600_000_000)
    half = keep + swapped(send)
    gram_part = exchange(half, PLANE)
    panels = jnp.where(col == 0, matrix, up + down)
    up = lax.ppermute(panels, "col", [(0, 1), (3, 4), (5, 6)])
    down = lax.ppermute(panels, "col", [(0, 7), (3, 2)])
    gram_part = exchange(spread(gram_part.sum(axis=0), lax.axis_size("col")), "col")
    own = exchange(spread(gram_part[0], lax.axis_size("y")), "y")
    panels = jnp.where((col == 0) | (col == 3) | (col == 5), panels, up + down)
    panels = lax.optimization_barrier(panels)
    products = inner(panels, matrix).reshape(2, -1, WIDE)
    mine = jnp.where(core == 0, products[0], products[1])
    half = mine + swapped(jnp.where(core == 0, products[1], products[0]))
    half, own = lax.optimization_barrier((half, own))
    part = exchange(half.reshape(chips, -1, WIDE), PLANE)
    own = gathered_along_x(own)
    (state,) = call(start_kernel, (which, own, swapped(own)), [(WIDE, WIDE)], 1_000_000_000)
    part, state = lax.optimization_barrier((part, state))
    half = exchange(spread(part.sum(axis=0), chips), PLANE).reshape(-1, WIDE)
    (inverse,) = call(finish_kernel, (state,), [(WIDE, WIDE)], 1_000_000_000)
    basis = product(panels, inverse.T) * math.sqrt(rows_all)
    half, basis = lax.optimization_barrier((half, basis))
    first, second = inverse[:, :PANEL], inverse[:, PANEL:]
    there = swapped(half)
    top = product(jnp.where(core == 0, first, second), half)
    top = top + product(jnp.where(core == 0, second, first), there)
    row = lax.broadcasted_iota(jnp.int32, (WIDE, WIDE), 0)
    column = lax.broadcasted_iota(jnp.int32, (WIDE, WIDE), 1)
    top = jnp.where((row > column) & (col == 0), 0.0, top)
    return (top, basis)


def solution(mesh):
    finer = Mesh(
        mesh.devices.reshape(4, 8, 2, mesh.shape["col"]), ("x", "y", "core", "col")
    )
    return jax.shard_map(
        steps,
        mesh=finer,
        in_specs=(P(ROW, "col"),),
        out_specs=(P(None, "col"), P(ROW, None)),
        check_vma=False,
    )
```

```python
import math

import jax
import jax.numpy as jnp
from jax import lax
from jax.experimental import pallas as pl
from jax.experimental.pallas import tpu as pltpu
from jax.sharding import Mesh
from jax.sharding import PartitionSpec as P


PANEL = 256
WIDE = 2 * PANEL
TILE = 128
STEP = 32
ROW = ("x", "y", "core")
PLANE = ("x", "y")
HIGHEST = lax.Precision.HIGHEST


def inner(left, right):
    return lax.dot_general(
        left,
        right,
        (((0,), (0,)), ((), ())),
        precision=HIGHEST,
        preferred_element_type=jnp.float32,
    )


def product(left, right):
    return jnp.dot(left, right, precision=HIGHEST, preferred_element_type=jnp.float32)


PLACES = {
    (0, 0): (0, 0), (0, 1): (0, 1), (0, 2): (0, 2), (0, 3): (0, 3), (3, 3): (0, 4),
    (1, 1): (1, 0), (1, 2): (1, 1), (1, 3): (1, 2), (2, 2): (1, 3), (2, 3): (1, 4),
}
NARROW = 5 * TILE


def span(place):
    return slice(place * TILE, (place + 1) * TILE)


def gram_kernel(core_ref, panels_ref, keep_ref, send_ref):
    for i in range(4):
        line = inner(panels_ref[:, span(i)], panels_ref[:, i * TILE :])
        half = PLACES[i, i][0]

        def put(ref):
            for j in range(i, 4):
                block = line[:, span(j - i)]
                ref[:, :, span(PLACES[i, j][1])] = block.reshape(*ref.shape[:2], TILE)

        @pl.when(core_ref[0] == half)
        def _():
            put(keep_ref)

        @pl.when(core_ref[0] != half)
        def _():
            put(send_ref)


def start_kernel(core_ref, own_ref, other_ref, out_ref):
    for half in range(2):

        def take(ref):
            for (i, j), (where, place) in PLACES.items():
                if where == half:
                    out_ref[span(i), span(j)] = ref[:, :, span(place)].reshape(TILE, TILE)

        @pl.when(core_ref[0] == half)
        def _():
            take(own_ref)

        @pl.when(core_ref[0] != half)
        def _():
            take(other_ref)

    factor_tiles(out_ref, 0, 1)


def finish_kernel(state_ref, out_ref):
    out_ref[...] = state_ref[...]
    factor_tiles(out_ref, 1, 4)
    row = lax.broadcasted_iota(jnp.int32, (WIDE, WIDE), 0)
    col = lax.broadcasted_iota(jnp.int32, (WIDE, WIDE), 1)
    out_ref[...] = jnp.where(col <= row, out_ref[...], 0.0)


def factor_tiles(out_ref, begin, end):
    row8 = lax.broadcasted_iota(jnp.int32, (8, TILE), 0)
    lane = lax.broadcasted_iota(jnp.int32, (8, TILE), 1)
    tiles, groups = WIDE // TILE, STEP // 8

    def outer(t, _):
        base = pl.multiple_of(t * TILE, TILE)
        for u in range(TILE // STEP):
            first = pl.multiple_of(base + u * STEP, STEP)
            block = out_ref[pl.ds(first, STEP), pl.ds(base, TILE)]
            cols = []
            for q in range(STEP):
                spread = jnp.broadcast_to(block[:, u * STEP + q : u * STEP + q + 1], (STEP, TILE))
                cols.append([spread[8 * v : 8 * v + 8] for v in range(groups)])
            rows = []
            for v in range(groups):
                rows.append([])
                for w in range(tiles):
                    values = out_ref[pl.ds(first + 8 * v, 8), TILE * w : TILE * (w + 1)]
                    here = (lane >= u * STEP) & (lane < (u + 1) * STEP) & (t == w)
                    unit = jnp.where(lane - u * STEP == row8 + 8 * v, 1.0, 0.0)
                    rows[v].append(jnp.where(here, unit, values))
            pivots = [None] * groups
            for k in range(STEP):
                vk, sk = k // 8, k % 8
                pivot = jnp.broadcast_to(cols[k][vk][sk : sk + 1], (8, TILE))
                inverse = 1.0 / pivot
                pivots[vk] = pivot if sk == 0 else jnp.where(row8 == sk, pivot, pivots[vk])
                scaled = {}
                for v in range(vk, groups):
                    s = cols[k][v] * inverse
                    scaled[v] = jnp.where(row8 > sk, s, 0.0) if v == vk else s
                for j in range(k + 1, STEP):
                    other = jnp.broadcast_to(cols[k][j // 8][j % 8 : j % 8 + 1], (8, TILE))
                    for v in range(j // 8, groups):
                        cols[j][v] = cols[j][v] - scaled[v] * other
                for w in range(tiles):
                    other = jnp.broadcast_to(rows[vk][w][sk : sk + 1], (8, TILE))
                    for v in range(vk, groups):
                        rows[v][w] = rows[v][w] - scaled[v] * other
            for v in range(groups):
                scale = lax.rsqrt(pivots[v])
                for w in range(tiles):
                    out_ref[pl.ds(first + 8 * v, 8), TILE * w : TILE * (w + 1)] = rows[v][w] * scale
            if u < TILE // STEP - 1:
                rest = TILE - (u + 1) * STEP
                done = out_ref[pl.ds(first, STEP), :]
                left = out_ref[pl.ds(first, STEP), pl.ds(base, TILE)][:, (u + 1) * STEP :]
                old = out_ref[pl.ds(first + STEP, rest), :]
                col = lax.broadcasted_iota(jnp.int32, (rest, WIDE), 1)
                old = jnp.where((col >= first) & (col < first + STEP), 0.0, old)
                out_ref[pl.ds(first + STEP, rest), :] = old - inner(left, done)

        done = out_ref[pl.ds(base, TILE), :]
        row = lax.broadcasted_iota(jnp.int32, (TILE, WIDE), 0) + base
        col = lax.broadcasted_iota(jnp.int32, (TILE, WIDE), 1)
        done = jnp.where((col <= row) | (col >= base + TILE), done, 0.0)

        def below(i, _):
            start = pl.multiple_of(i * TILE, TILE)
            old = out_ref[pl.ds(start, TILE), :]
            old = jnp.where((col >= base) & (col < base + TILE), 0.0, old)
            out_ref[pl.ds(start, TILE), :] = old - inner(
                out_ref[pl.ds(base, TILE), pl.ds(start, TILE)], done
            )
            return 0

        lax.fori_loop(t + 1, tiles, below, 0)
        return 0

    lax.fori_loop(begin, end, outer, 0)


def call(kernel, operands, shapes, flops):
    vmem, smem = pl.BlockSpec(memory_space=pltpu.VMEM), pl.BlockSpec(memory_space=pltpu.SMEM)
    return pl.pallas_call(
        kernel,
        out_shape=[jax.ShapeDtypeStruct(shape, jnp.float32) for shape in shapes],
        in_specs=[smem if a.ndim == 1 else vmem for a in operands],
        out_specs=[vmem for _ in shapes],
        compiler_params=pltpu.CompilerParams(vmem_limit_bytes=16 * 2**20),
        cost_estimate=pl.CostEstimate(flops=flops, bytes_accessed=2**21, transcendentals=0),
    )(*operands)


def exchange(blocks, axis):
    return lax.all_to_all(blocks, axis, 0, 0, tiled=True)


def spread(array, count):
    return jnp.broadcast_to(array[None], (count, *array.shape))


def swapped(array):
    return lax.ppermute(array, "core", [(0, 1), (1, 0)])


def steps(matrix):
    rows_all = matrix.shape[0] * lax.axis_size(ROW)
    chips = lax.axis_size(PLANE)
    core = lax.axis_index("core")
    which = core.reshape(1)
    col = lax.axis_index("col")

    up = lax.ppermute(matrix, "col", [(0, 3)])
    down = lax.ppermute(matrix, "col", [(0, 5)])
    keep, send = call(gram_kernel, (which, matrix), [(chips, TILE // chips, NARROW)] * 2, 600_000_000)
    half = keep + swapped(send)
    gram_part = exchange(half, PLANE)
    panels = jnp.where(col == 0, matrix, up + down)
    up = lax.ppermute(panels, "col", [(0, 1), (3, 4), (5, 6)])
    down = lax.ppermute(panels, "col", [(0, 7), (3, 2)])
    gram_part = exchange(spread(gram_part.sum(axis=0), lax.axis_size("col")), "col")
    own = exchange(spread(gram_part[0], chips), PLANE)
    panels = jnp.where((col == 0) | (col == 3) | (col == 5), panels, up + down)
    panels = lax.optimization_barrier(panels)
    products = inner(panels, matrix).reshape(2, -1, WIDE)
    mine = jnp.where(core == 0, products[0], products[1])
    half = mine + swapped(jnp.where(core == 0, products[1], products[0]))
    half, own = lax.optimization_barrier((half, own))
    part = exchange(half.reshape(chips, -1, WIDE), PLANE)
    (state,) = call(start_kernel, (which, own, swapped(own)), [(WIDE, WIDE)], 1_000_000_000)
    part, state = lax.optimization_barrier((part, state))
    half = exchange(spread(part.sum(axis=0), chips), PLANE).reshape(-1, WIDE)
    (inverse,) = call(finish_kernel, (state,), [(WIDE, WIDE)], 1_000_000_000)
    basis = product(panels, inverse.T) * math.sqrt(rows_all)
    half, basis = lax.optimization_barrier((half, basis))
    first, second = inverse[:, :PANEL], inverse[:, PANEL:]
    there = swapped(half)
    top = product(jnp.where(core == 0, first, second), half)
    top = top + product(jnp.where(core == 0, second, first), there)
    row = lax.broadcasted_iota(jnp.int32, (WIDE, WIDE), 0)
    column = lax.broadcasted_iota(jnp.int32, (WIDE, WIDE), 1)
    top = jnp.where((row > column) & (col == 0), 0.0, top)
    return (top, basis)


def solution(mesh):
    finer = Mesh(
        mesh.devices.reshape(4, 8, 2, mesh.shape["col"]), ("x", "y", "core", "col")
    )
    return jax.shard_map(
        steps,
        mesh=finer,
        in_specs=(P(ROW, "col"),),
        out_specs=(P(None, "col"), P(ROW, None)),
        check_vma=False,
    )
```
